256 devices in a mesh: groups: 2 (over z), seq: 128 (over y, x, core).
Axes of the slice: x: 8, y: 8, z: 2, core: 2. Of those that a mesh axis runs over, the one named last changes fastest.
The devices are a block of a 8x8x16 slice.
Arguments:
- hidden: bfloat16 [8192, 3072], P(('groups', 'seq')), parts along dimension 0, may hold values from -6 to 6
- queries: bfloat16 [8192, 3072], P(('groups', 'seq')), parts along dimension 0, may hold values from -6 to 6
- key_rows: bfloat16 [8192, 3072], P(('groups', 'seq')), parts along dimension 0, may hold values from -6 to 6
- values: bfloat16 [8192, 3072], P(('groups', 'seq')), parts along dimension 0, may hold values from -12 to 12
- query_gain: float32 [2, 128], replicated, may hold values from 0.6 to 5
- key_gain: float32 [2, 128], replicated, may hold values from 0.6 to 5
- gate_table: bfloat16 [64, 2, 3072], P('groups'), parts along dimension 0, may hold values from -6 to 6
- segment: int32 [8192], P(('groups', 'seq')), parts along dimension 0, may hold values from 0 to 31, as said below
- text_count: int32 [64], P('groups'), parts along dimension 0, may hold values from 1 to 64
Outputs:
- mixed: bfloat16 [8192, 3072], P(('groups', 'seq')), parts along dimension 0
The draws below stay inside these ranges and needn't reach their ends.
There are 2 independent parts, one for each index of `groups`. The reference program is written for one: setup_inputs(seed, part) draws one part's arguments, and reference() takes and returns one part's arrays. A program takes and returns all parts, laid end to end along the dimension named above; an argument that names none is the same for every part. Nothing has to cross between parts.
Inputs may be any that keep to these rules, and one draw needn't show every extreme that they name: `segment`: one device holds at most 2 tokens of one request; in every draw some two requests 2 j and 2 j + 1 get exactly 2 tokens from every device. Tokens of one request may lie anywhere on the devices.
All inputs are finite; a program needn't handle non-finite values.
Results may differ from the reference program's by a relative error of at most 0.012.
The reference program's roundings to bfloat16 on the way (of `query_normed`, `key_normed`, `weights` and `attention`) count: a program that leaves them out, or rounds other values in their place, can miss the bound.
Values may be sent and summed in bfloat16 or wider, within the bound.
A program may use at most 64 MiB of HBM per device.

```python
import math
import jax
import jax.numpy as jnp
from jax import lax

HEADS = 24
HEAD_DIM = 128
D = 3072
TOK_DEV = 32
TOKENS = 4096
FINE = 32
CAP = 2
REQS = 32
N_SEQ = 128


def layout(key):
    base_key = jax.random.fold_in(key, 7)
    devices = TOKENS // TOK_DEV
    pair_key, seat_key, bias_key = jax.random.split(base_key, 3)
    full_pair = jax.random.randint(pair_key, (), 0, FINE // 2) * 2
    seat_count = FINE * CAP
    seat_slice = jnp.arange(seat_count, dtype=jnp.int32) // CAP
    forced = seat_slice // 2 * 2 == full_pair
    slice_bias = jax.random.randint(bias_key, (FINE,), 0, 1 << 15)

    def one_device(device_key):
        score_key, order_key = jax.random.split(device_key)
        seat_score = (jax.random.randint(score_key, (seat_count,), 0, 1 << 16) + slice_bias[seat_slice]) * seat_count + jnp.arange(seat_count, dtype=jnp.int32)
        seat_score = jnp.where(forced, -1 - jnp.arange(seat_count, dtype=jnp.int32), seat_score)
        chosen = jnp.argsort(seat_score)[:TOK_DEV]
        token_order = jax.random.permutation(order_key, TOK_DEV)
        return seat_slice[chosen][token_order]
    fine_slice = jax.vmap(one_device)(jax.random.split(seat_key, devices)).reshape(TOKENS)
    segment = fine_slice
    return segment


def drawn(key):
    own_key = jax.random.fold_in(key, 11)
    query_key, key_key = jax.random.split(own_key, 2)
    queries = jnp.clip(jax.random.normal(query_key, (TOKENS, D), jnp.float32), -6.0, 6.0)
    key_data = jnp.clip(jax.random.normal(key_key, (TOKENS, D), jnp.float32), -6.0, 6.0)
    return (queries, key_data)


def draw_segment(key, part):
    return layout(key).astype(jnp.int32)


def draw_queries(key, part):
    return drawn(key)[0].astype(jnp.bfloat16)


def draw_key_rows(key, part):
    return drawn(key)[1].astype(jnp.bfloat16)


def gain_draw(key):
    return jax.random.uniform(key, (2, HEAD_DIM), jnp.float32, 0.6, 1.6)


def draw_query_gain(key, part):
    return gain_draw(jax.random.fold_in(key, 21))


def draw_key_gain(key, part):
    return gain_draw(jax.random.fold_in(key, 23))


def with_ends(values, stream_key, smallest, high):
    longest = values.shape.index(max(values.shape))
    spots = []
    for shift in (0, 1):
        where = [jax.random.randint(jax.random.fold_in(stream_key, axis), (), 0, length) for axis, length in enumerate(values.shape)]
        where[longest] = (where[longest] + shift) % values.shape[longest]
        spots.append(tuple(where))
    return values.at[spots[0]].set(smallest).at[spots[1]].set(high)


def steps_of(stream_key, shape, shards, smallest, top_value):
    def one(dim, parts):
        heights = jax.random.uniform(jax.random.fold_in(jax.random.fold_in(stream_key, 6), dim), (parts,), jnp.float32, smallest / len(shards), top_value / len(shards))
        return jnp.repeat(jnp.exp(heights), shape[dim] // parts).reshape((-1,) + (1,) * (len(shape) - dim - 1))

    loudness = one(*shards[0])
    for cut in shards[1:]:
        loudness = loudness * one(*cut)
    return loudness


def centred(key, shape, deviation, reach, cuts=(), held_as=jnp.bfloat16):
    loudness = steps_of(key, shape, cuts, -0.22, 0.18) if cuts else 1.0
    array = jax.random.normal(key, shape, jnp.float32) * deviation * loudness
    return jnp.minimum(jnp.maximum(array, -reach), reach).astype(held_as)


def setup_inputs(seed: int = 0, part: int = 0) -> dict:
    key_list = jax.random.split(jax.random.key(seed), 10)
    own_keys = jax.random.split(jax.random.fold_in(key_list[9], part), 10)
    hidden = centred(own_keys[0], (TOKENS, D), 1.0, 6.0, ((0, 128),))
    queries = draw_queries(jax.random.fold_in(jax.random.fold_in(key_list[9], part), 71), part)
    key_rows = draw_key_rows(jax.random.fold_in(jax.random.fold_in(key_list[9], part), 71), part)
    values = centred(own_keys[3], (TOKENS, D), 2.0, 12.0, ((0, 128),))
    query_gain = draw_query_gain(jax.random.fold_in(key_list[9], 71), part)
    key_gain = draw_key_gain(jax.random.fold_in(key_list[9], 71), part)
    gate_table = centred(own_keys[6], (REQS, 2, D), 1.0, 6.0)
    segment = draw_segment(jax.random.fold_in(jax.random.fold_in(key_list[9], part), 71), part)
    text_count = with_ends(jax.random.randint(own_keys[8], (REQS,), 1, N_SEQ * CAP // 4 + 1), jax.random.fold_in(own_keys[8], 1), 1, (N_SEQ * CAP // 4 + 1) - 1).astype(jnp.int32)
    return dict(hidden=hidden, queries=queries, key_rows=key_rows, values=values, query_gain=query_gain, key_gain=key_gain, gate_table=gate_table, segment=segment, text_count=text_count)


EPSILON = 1e-06
MASKED = -1e+30

def head_norm(rows_in, gains, stream):
    row_count = rows_in.shape[0]
    per_head = rows_in.astype(jnp.float32).reshape(row_count, -1, HEAD_DIM)
    inverse = lax.rsqrt(lax.optimization_barrier(jnp.mean(per_head * per_head, axis=-1, keepdims=True)) + EPSILON)
    gain_rows = jnp.where((stream == 0)[:, None], gains[0][None, :], gains[1][None, :])
    return (per_head * inverse * gain_rows[:, None, :]).astype(jnp.bfloat16).reshape(row_count, -1)

def attend(query_block, block_segment, key_data, value_data, key_segment):
    scores = jnp.einsum('qhd,khd->hqk', query_block.astype(jnp.float32), key_data.astype(jnp.float32)) * (1.0 / math.sqrt(HEAD_DIM))
    allowed = (block_segment[:, None] == key_segment[None, :])[None, :, :]
    scores = jnp.where(allowed, scores, MASKED)
    largest = lax.optimization_barrier(jnp.max(scores, axis=-1, keepdims=True))
    weights = jnp.exp(scores - largest)
    weights = (weights / lax.optimization_barrier(jnp.sum(weights, axis=-1, keepdims=True))).astype(jnp.bfloat16)
    return jnp.einsum('hqk,khd->qhd', weights.astype(jnp.float32), value_data.astype(jnp.float32)).astype(jnp.bfloat16)

def reference(hidden, queries, key_rows, values, query_gain, key_gain, gate_table, segment, text_count):
    requests = text_count.shape[0]
    seg_hot = (segment[:, None] == jnp.arange(requests, dtype=jnp.int32)[None, :]).astype(jnp.int32)
    position = lax.optimization_barrier(jnp.sum((jnp.cumsum(seg_hot, axis=0) - seg_hot) * seg_hot, axis=1))
    text_limit = lax.optimization_barrier(jnp.sum(seg_hot * text_count[None, :], axis=1))
    stream = (position >= text_limit).astype(jnp.int32)
    query_normed = head_norm(queries, query_gain, stream)
    key_normed = head_norm(key_rows, key_gain, stream)
    fine_slice = segment.astype(jnp.int32)
    fine_hot = (fine_slice[:, None] == jnp.arange(FINE, dtype=jnp.int32)[None, :]).astype(jnp.int32)
    slice_rank = lax.optimization_barrier(jnp.sum((jnp.cumsum(fine_hot, axis=0) - fine_hot) * fine_hot, axis=1))
    slice_width = N_SEQ * CAP
    slot_table = jnp.full((FINE, slice_width), TOKENS, jnp.int32).at[fine_slice, slice_rank].set(jnp.arange(TOKENS, dtype=jnp.int32))
    zero_row = jnp.zeros((1, D), jnp.bfloat16)
    query_padded = jnp.concatenate([query_normed, zero_row], axis=0)
    key_padded = jnp.concatenate([key_normed, zero_row], axis=0)
    value_padded = jnp.concatenate([values, zero_row], axis=0)
    segment_padded = jnp.concatenate([segment, jnp.full((1,), -1, jnp.int32)], axis=0)

    def one_slice(slot_index):
        query_slice = jnp.take(query_padded, slot_index, axis=0).reshape(slice_width, HEADS, HEAD_DIM)
        key_slice = jnp.take(key_padded, slot_index, axis=0).reshape(slice_width, HEADS, HEAD_DIM)
        value_slice = jnp.take(value_padded, slot_index, axis=0).reshape(slice_width, HEADS, HEAD_DIM)
        slot_segment = jnp.take(segment_padded, slot_index, axis=0)
        result = attend(query_slice, slot_segment, key_slice, value_slice, slot_segment)
        return result.reshape(slice_width, D)
    blocks = lax.map(one_slice, slot_table)
    attention = jnp.zeros((TOKENS + 1, D), jnp.bfloat16).at[slot_table.reshape(-1)].set(blocks.reshape(-1, D))[:TOKENS]
    gate_rows = jnp.take(gate_table.reshape(requests * 2, D), segment * 2 + stream, axis=0)
    mixed = hidden.astype(jnp.float32) + gate_rows.astype(jnp.float32) * attention.astype(jnp.float32)
    return mixed.astype(jnp.bfloat16)
```

```python
import functools
import math

import jax
import jax.numpy as jnp
from jax import lax
from jax.experimental import pallas as pl
from jax.experimental.pallas import tpu as pltpu
from jax.sharding import Mesh
from jax.sharding import PartitionSpec as P

HEAD_DIM = 128
LANES = 128
CORES = 2
EPSILON = 1e-06
MASKED = -1e30
Y, X, C = "seq_0", "seq_1", "seq_2"
GROUPS_SEQ = ("groups", Y, X, C)
MESH = pl.DeviceIdType.MESH
F32 = jnp.float32
BF16 = jnp.bfloat16


def kernel(
    ny, nx, tok,
    hidden_hbm, query_hbm, key_hbm, value_hbm, query_gain, key_gain, gate_hbm, seg_ref, text_ref,
    out_ref,
    hid, que, key, val, gat,
    kra, qra, krb, qrb, ka, va, kb, vb, qa, qb,
    segrow, segall, turned, cola, colb, stra, gates,
    ma, la, acca, mb, lb, accb, oa, ob, atta, attb,
    load_sem, seg_send, seg_recv, all_send, all_recv,
    a_send, a_recv, b_send, b_recv, ra_send, ra_recv, rb_send, rb_recv, d_send, d_recv,
    oa_send, oa_recv, ob_send, ob_recv,
):
    ha = nx * CORES
    row_tok = ha * tok
    per_row = LANES // tok
    lane_rows = row_tok // LANES
    y, x, c = lax.axis_index(Y), lax.axis_index(X), lax.axis_index(C)
    idx = x * CORES + c

    def row_peer(i):
        return lax.rem(idx + i, ha)

    def row_dev(j):
        return {Y: y, X: j // CORES, C: lax.rem(j, CORES)}

    def col_dev(j):
        return {Y: j, X: x, C: c}

    def around(a, n):
        return lax.rem(a + 2 * n, n)

    partner = {Y: y, X: x, C: 1 - c}

    barrier = pltpu.get_barrier_semaphore()

    @pl.loop(1, ha)
    def _(i):
        pl.semaphore_signal(barrier, inc=1, device_id=row_dev(row_peer(i)), device_id_type=MESH)

    @pl.loop(1, ny)
    def _(j):
        pl.semaphore_signal(barrier, inc=1, device_id=col_dev(lax.rem(y + j, ny)), device_id_type=MESH)

    loads = [
        pltpu.make_async_copy(src, dst, load_sem.at[n])
        for n, (src, dst) in enumerate(
            [(key_hbm, key), (value_hbm, val), (query_hbm, que), (hidden_hbm, hid), (gate_hbm, gat)]
        )
    ]
    for load in loads:
        load.start()
    segrow[pl.ds(idx, 1)] = seg_ref[...].reshape(1, 1, LANES)
    for load in loads[:3]:
        load.wait()
    pl.semaphore_wait(barrier, ha - 1 + ny - 1)

    def remote(src, dst, send, recv, dev):
        return pltpu.make_async_remote_copy(
            src_ref=src, dst_ref=dst, send_sem=send, recv_sem=recv, device_id=dev, device_id_type=MESH
        )

    def head(ref, h):
        return ref.at[:, pl.ds(pl.multiple_of(h * HEAD_DIM, HEAD_DIM), HEAD_DIM)]

    def head_value(ref, h):
        return ref[:, pl.ds(pl.multiple_of(h * HEAD_DIM, HEAD_DIM), HEAD_DIM)]

    def seg_copy(i, src_idx, dst_idx):
        return remote(
            segrow.at[src_idx], segrow.at[src_idx], seg_send.at[i], seg_recv.at[i], row_dev(dst_idx)
        )

    @pl.loop(1, ha)
    def _(i):
        seg_copy(i, idx, row_peer(i)).start()

    tensors = (key, val, que)

    def a_target(n, slot):
        return (kra.at[slot], va.at[y, slot], qra.at[slot])[n]

    def b_target(n, slot):
        return (krb.at[slot], vb.at[slot, idx], qrb.at[slot])[n]

    def a_copy(n, i, src_idx, dst_idx):
        return remote(
            head(tensors[n], dst_idx), a_target(n, src_idx), a_send.at[n, i], a_recv.at[n, i], row_dev(dst_idx)
        )

    def b_copy(n, j, src_y, dst_y):
        return remote(
            head(tensors[n], ha + dst_y), b_target(n, src_y), b_send.at[n, j], b_recv.at[n, j], col_dev(dst_y)
        )

    for n in range(3):

        @pl.loop(1, ha)
        def _(i):
            a_copy(n, i, idx, row_peer(i)).start()

        @pl.loop(1, ny)
        def _(j):
            b_copy(n, j, y, lax.rem(y + j, ny)).start()

    kra[pl.ds(idx, 1)] = head_value(key, idx)[None]
    qra[pl.ds(idx, 1)] = head_value(que, idx)[None]
    va[pl.ds(y, 1), pl.ds(idx, 1)] = head_value(val, idx)[None, None]
    krb[pl.ds(y, 1)] = head_value(key, ha + y)[None]
    qrb[pl.ds(y, 1)] = head_value(que, ha + y)[None]
    vb[pl.ds(y, 1), pl.ds(idx, 1)] = head_value(val, ha + y)[None, None]

    def a_wait(n):
        @pl.loop(1, ha)
        def _(i):
            a_copy(n, i, lax.rem(idx + ha - i, ha), idx).wait_recv()

    def b_wait(n):
        @pl.loop(1, ny)
        def _(j):
            b_copy(n, j, lax.rem(y + ny - j, ny), y).wait_recv()

    @pl.loop(1, ha)
    def _(i):
        seg_copy(i, lax.rem(idx + ha - i, ha), idx).wait_recv()

    lane = lax.broadcasted_iota(jnp.int32, (1, LANES), 1)
    for r in range(lane_rows):
        joined = segrow[per_row * r]
        for g in range(1, per_row):
            joined = jnp.where(lane >= g * tok, segrow[per_row * r + g], joined)
        segall[pl.ds(y, 1), r : r + 1, :] = joined[None]

    def all_copy(j, src_y, dst_y):
        return remote(segall.at[src_y], segall.at[src_y], all_send.at[j], all_recv.at[j], col_dev(dst_y))

    @pl.loop(1, ny)
    def _(j):
        all_copy(j, y, lax.rem(y + j, ny)).start()

    def turn(row):
        return jnp.broadcast_to(row, (LANES, LANES)).T

    for r in range(lane_rows):
        cola[r * LANES : (r + 1) * LANES, :] = turn(segall[pl.ds(y, 1), r : r + 1, :].reshape(1, LANES))

    @pl.loop(1, ny)
    def _(j):
        all_copy(j, lax.rem(y + ny - j, ny), y).wait_recv()

    my_row, my_part = idx // per_row, lax.rem(idx, per_row)
    for yy in range(ny):
        turned[...] = turn(segall[yy, pl.ds(my_row, 1), :])
        colb[yy * tok : (yy + 1) * tok, :] = turned[pl.ds(pl.multiple_of(my_part * tok, tok), tok), :]

    def stream_of(col, order):
        rows = col.shape[0]

        def add(yy, count):
            for r in range(lane_rows):
                other = segall[yy, r : r + 1, :]
                place = yy * row_tok + r * LANES + lane
                count = count + jnp.where((col == other) & (place < order), 1.0, 0.0)
            return count

        count = lax.fori_loop(0, ny, add, jnp.zeros((rows, LANES), F32))
        position = jnp.sum(count, axis=1, keepdims=True)
        limit = jnp.sum(jnp.where(col == lane.astype(F32), text_ref[...], 0.0), axis=1, keepdims=True)
        return jnp.where(position >= limit, 1.0, 0.0)

    def normed(rows_in, gains, stream):
        wide = rows_in.astype(F32)
        inverse = lax.rsqrt(jnp.mean(wide * wide, axis=1, keepdims=True) + EPSILON)
        gain_rows = jnp.where(stream == 0.0, gains[0:1, :], gains[1:2, :])
        return (wide * inverse * gain_rows).astype(BF16)

    a_wait(0)
    for r in range(lane_rows):
        rows = pl.ds(r * LANES, LANES)
        slots = pl.ds(r * per_row, per_row)
        order = y * row_tok + r * LANES + lax.broadcasted_iota(jnp.int32, (LANES, LANES), 0)
        stream = stream_of(cola[rows, :], order)
        stra[rows, :] = jnp.broadcast_to(stream, (LANES, LANES))
        fresh = normed(kra[slots].reshape(LANES, HEAD_DIM), key_gain, stream)
        ka[pl.ds(y, 1), slots] = fresh.reshape(1, per_row, tok, HEAD_DIM)

    full = ny // 2 - 1
    full_x = nx // 2 - 1

    def a_part(buf, slot, way, whole):
        if whole:
            return buf.at[slot]
        return buf.at[slot, pl.ds(way * (ha // 2), ha // 2)]

    def b_part(buf, slot, way, whole):
        if whole:
            return buf.at[:, slot]
        return buf.at[pl.ds(way * (ny // 2), ny // 2), slot]

    def a_ring(t, way, s, arriving):
        buf = (ka, va)[t]
        sign = 1 if way == 0 else -1
        back = s + 1 if arriving else s
        part = a_part(buf, around(y - sign * back, ny), way, s < full)
        return remote(
            part, part, ra_send.at[t, way, s], ra_recv.at[t, way, s], col_dev(around(y + sign, ny))
        )

    def b_ring(t, way, s, arriving):
        buf = (kb, vb)[t]
        sign = 1 if way == 0 else -1
        back = s + 1 if arriving else s
        slot = around(x - sign * back, nx) * CORES + c
        part = b_part(buf, slot, way, s < full_x)
        dev = {Y: y, X: around(x + sign, nx), C: c}
        return remote(part, part, rb_send.at[t, way, s], rb_recv.at[t, way, s], dev)

    def d_copy(t, way, s, core):
        buf = (kb, vb)[t]
        sign = 1 if way == 0 else -1
        if s < 0:
            part = buf.at[:, x * CORES + core]
        else:
            slot = around(x - sign * (s + 1), nx) * CORES + core
            part = b_part(buf, slot, way, s < full_x)
        n = 0 if s < 0 else 1 + 2 * s + way
        return remote(part, part, d_send.at[t, n], d_recv.at[t, n], partner)

    ways = (0, 1)
    for way in ways:
        a_ring(0, way, 0, False).start()

    b_wait(0)
    order_b = lax.broadcasted_iota(jnp.int32, (ny * tok, LANES), 0)
    order_b = order_b // tok * row_tok + idx * tok + lax.rem(order_b, tok)
    stream_b = stream_of(colb[...], order_b)
    kb[:, pl.ds(idx, 1)] = normed(krb[...].reshape(ny * tok, HEAD_DIM), key_gain, stream_b).reshape(
        ny, 1, tok, HEAD_DIM
    )
    for way in ways:
        b_ring(0, way, 0, False).start()
    d_copy(0, 0, -1, c).start()

    a_wait(1)
    for way in ways:
        a_ring(1, way, 0, False).start()
    b_wait(1)
    for way in ways:
        b_ring(1, way, 0, False).start()
    d_copy(1, 0, -1, c).start()

    a_wait(2)
    for r in range(lane_rows):
        rows = pl.ds(r * LANES, LANES)
        slots = pl.ds(r * per_row, per_row)
        qa[rows, :] = normed(qra[slots].reshape(LANES, HEAD_DIM), query_gain, stra[rows, 0:1])
    b_wait(2)
    qb[...] = normed(qrb[...].reshape(ny * tok, HEAD_DIM), query_gain, stream_b)

    for m, l, acc in ((ma, la, acca), (mb, lb, accb)):
        m[...] = jnp.full(m.shape, MASKED, F32)
        l[...] = jnp.zeros(l.shape, F32)
        acc[...] = jnp.zeros(acc.shape, F32)

    scale = 1.0 / math.sqrt(HEAD_DIM)

    def attend(q, cols, m, l, acc, keys, vals, slot):
        block = LANES

        @pl.loop(0, q.shape[0] // block)
        def _(b):
            rows = pl.ds(pl.multiple_of(b * block, block), block)
            kk = keys[slot].reshape(row_tok, HEAD_DIM)
            vv = vals[slot].reshape(row_tok, HEAD_DIM)
            s = lax.dot_general(q[rows, :], kk, (((1,), (1,)), ((), ())), preferred_element_type=F32) * scale
            mine = cols[rows, :]
            parts = []
            for r in range(lane_rows):
                other = segall[slot, r : r + 1, :]
                parts.append(jnp.where(mine == other, s[:, r * LANES : (r + 1) * LANES], MASKED))
            top = parts[0]
            for part in parts[1:]:
                top = jnp.maximum(top, part)
            old = m[rows, :]
            new = jnp.maximum(old, jnp.max(top, axis=1, keepdims=True))
            shrink = jnp.exp(old - new)
            parts = [jnp.exp(part - new) for part in parts]
            total = parts[0]
            for part in parts[1:]:
                total = total + part
            m[rows, :] = new
            l[rows, :] = l[rows, :] * shrink + total
            weights = jnp.concatenate([part.astype(BF16) for part in parts], axis=1)
            acc[rows, :] = acc[rows, :] * shrink + jnp.dot(weights, vv, preferred_element_type=F32)

    def attend_a(slot):
        attend(qa, cola, ma, la, acca, ka, va, slot)

    attend_a(y)

    for load in loads[3:]:
        load.wait()
    own = pl.ds(pl.multiple_of(idx * tok, tok), tok)
    entry = cola[own, :] * 2.0 + stra[own, :]
    pick = jnp.where(entry == lane.astype(F32), 1.0, 0.0).astype(BF16)[:, : gat.shape[0]]
    gates[...] = jnp.dot(pick, gat[...], preferred_element_type=F32)

    steps = max(full, full_x) + 1
    for s in range(steps):
        in_a, in_b = s <= full, s <= full_x
        for t in (0, 1):
            if in_b:
                for way in ways:
                    b_ring(t, way, s, True).wait_recv()
                    if s < full_x:
                        b_ring(t, way, s + 1, False).start()
                    d_copy(t, way, s, c).start()
            if in_a and s < full:
                for way in ways:
                    a_ring(t, way, s, True).wait_recv()
                    a_ring(t, way, s + 1, False).start()
        if s < full:
            attend_a(around(y - s - 1, ny))
            attend_a(around(y + s + 1, ny))

    for t in (0, 1):
        d_copy(t, 0, -1, 1 - c).wait_recv()
        for s in range(full_x + 1):
            for way in ways:
                d_copy(t, way, s, 1 - c).wait_recv()

    @pl.loop(0, ny)
    def _(slot):
        attend(qb, colb, mb, lb, accb, kb, vb, slot)

    def finish(l, acc):
        return (acc[...] / jnp.sum(l[...], axis=1, keepdims=True)).astype(BF16)

    ob[...] = finish(lb, accb).reshape(ny, tok, HEAD_DIM)

    def ob_copy(j, src_y, dst_y):
        return remote(ob.at[dst_y], attb.at[src_y], ob_send.at[j], ob_recv.at[j], col_dev(dst_y))

    @pl.loop(1, ny)
    def _(j):
        ob_copy(j, y, lax.rem(y + j, ny)).start()

    attb[pl.ds(y, 1)] = ob[pl.ds(y, 1)]

    for t in (0, 1):
        for way in ways:
            a_ring(t, way, full, True).wait_recv()
    attend_a(around(y + ny // 2, ny))
    oa[...] = finish(la, acca).reshape(ha, tok, HEAD_DIM)

    def oa_copy(i, src_idx, dst_idx):
        return remote(oa.at[dst_idx], atta.at[src_idx], oa_send.at[i], oa_recv.at[i], row_dev(dst_idx))

    @pl.loop(1, ha)
    def _(i):
        oa_copy(i, idx, row_peer(i)).start()

    atta[pl.ds(idx, 1)] = oa[pl.ds(idx, 1)]

    @pl.loop(1, ha)
    def _(i):
        seg_copy(i, idx, row_peer(i)).wait_send()
        for n in range(3):
            a_copy(n, i, idx, row_peer(i)).wait_send()

    @pl.loop(1, ny)
    def _(j):
        all_copy(j, y, lax.rem(y + j, ny)).wait_send()
        for n in range(3):
            b_copy(n, j, y, lax.rem(y + j, ny)).wait_send()

    for t in (0, 1):
        d_copy(t, 0, -1, c).wait_send()
        for way in ways:
            for s in range(full + 1):
                a_ring(t, way, s, False).wait_send()
            for s in range(full_x + 1):
                b_ring(t, way, s, False).wait_send()
                d_copy(t, way, s, c).wait_send()

    @pl.loop(1, ny)
    def _(j):
        ob_copy(j, lax.rem(y + ny - j, ny), y).wait_recv()

    @pl.loop(1, ha)
    def _(i):
        oa_copy(i, lax.rem(idx + ha - i, ha), idx).wait_recv()

    for h in range(ha + ny):
        columns = slice(h * HEAD_DIM, (h + 1) * HEAD_DIM)
        result = atta[h] if h < ha else attb[h - ha]
        out_ref[:, columns] = (
            hid[:, columns].astype(F32) + gates[:, columns] * result.astype(F32)
        ).astype(BF16)

    @pl.loop(1, ny)
    def _(j):
        ob_copy(j, y, lax.rem(y + j, ny)).wait_send()

    @pl.loop(1, ha)
    def _(i):
        oa_copy(i, idx, row_peer(i)).wait_send()


def per_device(
    ny, nx, hidden, queries, key_rows, values, query_gain, key_gain, gate_table, segment, text_count
):
    tok, width = hidden.shape
    requests = text_count.shape[0]
    ha = nx * CORES
    row_tok = ha * tok
    seg_row = jnp.tile(segment, LANES // tok)[None, :].astype(F32)
    text_row = jnp.pad(text_count, (0, LANES - requests))[None, :].astype(F32)
    gate_rows = gate_table.reshape(2 * requests, width)
    anywhere = pl.BlockSpec(memory_space=pl.ANY)
    vmem = pl.BlockSpec(memory_space=pltpu.VMEM)
    dma = pltpu.SemaphoreType.DMA
    heads = (tok, HEAD_DIM)
    half_y, half_x = ny // 2, nx // 2
    return pl.pallas_call(
        functools.partial(kernel, ny, nx, tok),
        out_shape=jax.ShapeDtypeStruct((tok, width), BF16),
        in_specs=[anywhere] * 4 + [vmem] * 2 + [anywhere] + [vmem] * 2,
        out_specs=vmem,
        scratch_shapes=[
            pltpu.VMEM((tok, width), BF16),
            pltpu.VMEM((tok, width), BF16),
            pltpu.VMEM((tok, width), BF16),
            pltpu.VMEM((tok, width), BF16),
            pltpu.VMEM((2 * requests, width), BF16),
            pltpu.VMEM((ha, *heads), BF16),
            pltpu.VMEM((ha, *heads), BF16),
            pltpu.VMEM((ny, *heads), BF16),
            pltpu.VMEM((ny, *heads), BF16),
            pltpu.VMEM((ny, ha, *heads), BF16),
            pltpu.VMEM((ny, ha, *heads), BF16),
            pltpu.VMEM((ny, ha, *heads), BF16),
            pltpu.VMEM((ny, ha, *heads), BF16),
            pltpu.VMEM((row_tok, HEAD_DIM), BF16),
            pltpu.VMEM((ny * tok, HEAD_DIM), BF16),
            pltpu.VMEM((ha, 1, LANES), F32),
            pltpu.VMEM((ny, 8, LANES), F32),
            pltpu.VMEM((LANES, LANES), F32),
            pltpu.VMEM((row_tok, LANES), F32),
            pltpu.VMEM((ny * tok, LANES), F32),
            pltpu.VMEM((row_tok, LANES), F32),
            pltpu.VMEM((tok, width), F32),
            pltpu.VMEM((row_tok, LANES), F32),
            pltpu.VMEM((row_tok, LANES), F32),
            pltpu.VMEM((row_tok, HEAD_DIM), F32),
            pltpu.VMEM((ny * tok, LANES), F32),
            pltpu.VMEM((ny * tok, LANES), F32),
            pltpu.VMEM((ny * tok, HEAD_DIM), F32),
            pltpu.VMEM((ha, *heads), BF16),
            pltpu.VMEM((ny, *heads), BF16),
            pltpu.VMEM((ha, *heads), BF16),
            pltpu.VMEM((ny, *heads), BF16),
            dma((5,)),
            dma((ha,)),
            dma((ha,)),
            dma((ny,)),
            dma((ny,)),
            dma((3, ha)),
            dma((3, ha)),
            dma((3, ny)),
            dma((3, ny)),
            dma((2, 2, half_y)),
            dma((2, 2, half_y)),
            dma((2, 2, half_x)),
            dma((2, 2, half_x)),
            dma((2, 1 + 2 * half_x)),
            dma((2, 1 + 2 * half_x)),
            dma((ha,)),
            dma((ha,)),
            dma((ny,)),
            dma((ny,)),
        ],
        compiler_params=pltpu.CompilerParams(
            collective_id=0, has_side_effects=True, vmem_limit_bytes=40 * 1024 * 1024
        ),
        name="joint_attention",
    )(hidden, queries, key_rows, values, query_gain, key_gain, gate_rows, seg_row, text_row)


def solution(mesh):
    groups, seq = mesh.shape["groups"], mesh.shape["seq"]
    nx = math.isqrt(seq // CORES)
    ny = seq // CORES // nx
    finer = Mesh(mesh.devices.reshape(groups, ny, nx, CORES), GROUPS_SEQ)
    placed = (
        P(GROUPS_SEQ, None),
        P(GROUPS_SEQ, None),
        P(GROUPS_SEQ, None),
        P(GROUPS_SEQ, None),
        P(),
        P(),
        P("groups", None, None),
        P(GROUPS_SEQ),
        P("groups"),
    )
    return jax.shard_map(
        functools.partial(per_device, ny, nx),
        mesh=finer,
        in_specs=placed,
        out_specs=P(GROUPS_SEQ, None),
        check_vma=False,
    )
```

```python
import functools
import math

import jax
import jax.numpy as jnp
from jax import lax
from jax.experimental import pallas as pl
from jax.experimental.pallas import tpu as pltpu
from jax.sharding import Mesh
from jax.sharding import PartitionSpec as P

HEAD_DIM = 128
LANES = 128
CORES = 2
EPSILON = 1e-06
LOWEST = -1e30
SAME = (128.0, 64.0)
LATER = 64.0
BLOCK = 256
VMEM_BYTES = 60 * 1024 * 1024
Y, X, C = "seq_0", "seq_1", "seq_2"
GROUPS_SEQ = ("groups", Y, X, C)
MESH = pl.DeviceIdType.MESH
F32 = jnp.float32
BF16 = jnp.bfloat16


def kernel(
    ny, nx, tok, requests,
    hidden_hbm, query_hbm, key_hbm, value_hbm, query_gain, key_gain, gate_hbm, seg_ref, text_ref,
    out_ref,
    hid, que, key, val, gat,
    kra, qra, krb, qrb, ka, va, kb, vb, qa, qb,
    segrow, segall, codea, codeb, tri, hot, cola, gains, gates, kwork, held,
    ma, la, acca, mb, lb, accb, oa, ob, atta, attb,
    load_sem, seg_send, seg_recv, all_send, all_recv,
    a_send, a_recv, b_send, b_recv, ra_send, ra_recv, rb_send, rb_recv, d_send, d_recv,
    oa_send, oa_recv, ob_send, ob_recv,
):
    ha = nx * CORES
    row_tok, col_tok = ha * tok, ny * tok
    per = LANES // tok
    a_rows, b_rows = row_tok // LANES, col_tok // LANES
    y, x, c = lax.axis_index(Y), lax.axis_index(X), lax.axis_index(C)
    idx = x * CORES + c
    ways = (0, 1)

    loads = [
        pltpu.make_async_copy(src, dst, load_sem.at[n])
        for n, (src, dst) in enumerate(
            [(key_hbm, key), (value_hbm, val), (query_hbm, que), (hidden_hbm, hid), (gate_hbm, gat)]
        )
    ]
    for load in loads:
        load.start()

    def around(a, n):
        return lax.rem(a + 2 * n, n)

    row = []
    for dx in range(nx):
        for dc in range(CORES):
            if dx or dc:
                xx = around(x + dx, nx)
                cc = c if dc == 0 else 1 - c
                row.append((xx * CORES + cc, {Y: y, X: xx, C: cc}))
    col = []
    for dy in range(1, ny):
        yy = around(y + dy, ny)
        col.append((yy, {Y: yy, X: x, C: c}))
    partner = {Y: y, X: x, C: 1 - c}

    barrier = pltpu.get_barrier_semaphore()
    for _, dev in row + col:
        pl.semaphore_signal(barrier, inc=1, device_id=dev, device_id_type=MESH)

    lane = lax.broadcasted_iota(jnp.int32, (1, LANES), 1)
    lane_f = lane.astype(F32)
    place = lax.rem(lane, tok)
    mine = jnp.zeros((1, LANES), F32)
    for i in range(tok):
        mine = jnp.where(place == i, seg_ref[i].astype(F32), mine)
    segrow[pl.ds(idx, 1)] = mine.reshape(1, 1, LANES)
    down = lax.broadcasted_iota(jnp.int32, (requests, LANES), 0)
    limit = jnp.zeros((requests, LANES), F32)
    for i in range(requests):
        limit = jnp.where(down == i, text_ref[i].astype(F32), limit)
    down = down.astype(F32)
    deep = lax.broadcasted_iota(jnp.int32, (LANES, LANES), 0).astype(F32)
    for r in range(a_rows):
        first = lax.broadcasted_iota(jnp.int32, (LANES, row_tok), 0) + r * LANES
        second = lax.broadcasted_iota(jnp.int32, (LANES, row_tok), 1)
        tri[r * LANES : (r + 1) * LANES, :] = jnp.where(first < second, 1.0, 0.0).astype(BF16)

    def turn(line):
        return jnp.broadcast_to(line, (LANES, LANES)).T

    for i in range(2):
        gains[i] = turn(key_gain[i : i + 1, :])
    for m, l, acc in ((ma, la, acca), (mb, lb, accb)):
        m[...] = jnp.full(m.shape, LOWEST, F32)
        l[...] = jnp.zeros(l.shape, F32)
        acc[...] = jnp.zeros(acc.shape, F32)

    loads[0].wait()
    pl.semaphore_wait(barrier, len(row) + len(col))

    def remote(src, dst, send, recv, dev):
        return pltpu.make_async_remote_copy(
            src_ref=src, dst_ref=dst, send_sem=send, recv_sem=recv, device_id=dev, device_id_type=MESH
        )

    def head(ref, h):
        return ref.at[:, pl.ds(pl.multiple_of(h * HEAD_DIM, HEAD_DIM), HEAD_DIM)]

    def head_value(ref, h):
        return ref[:, pl.ds(pl.multiple_of(h * HEAD_DIM, HEAD_DIM), HEAD_DIM)]

    def wait_all(ref, sem):
        pltpu.make_async_copy(ref, ref, sem).wait()

    tensors = (key, val, que)
    a_in = (kra, va.at[y], qra)
    b_in = (krb, vb.at[idx], qrb)

    def a_start(n):
        for j, dev in row:
            remote(head(tensors[n], j), a_in[n].at[idx], a_send.at[n], a_recv.at[n], dev).start()

    def b_start(n):
        for j, dev in col:
            remote(head(tensors[n], ha + j), b_in[n].at[y], b_send.at[n], b_recv.at[n], dev).start()

    a_start(0)
    for _, dev in row:
        remote(segrow.at[idx], segrow.at[idx], seg_send, seg_recv, dev).start()
    for n in range(3):
        if n:
            loads[n].wait()
        b_start(n)

    kra[pl.ds(idx, 1)] = head_value(key, idx)[None]
    qra[pl.ds(idx, 1)] = head_value(que, idx)[None]
    va[pl.ds(y, 1), pl.ds(idx, 1)] = head_value(val, idx)[None, None]
    krb[pl.ds(y, 1)] = head_value(key, ha + y)[None]
    qrb[pl.ds(y, 1)] = head_value(que, ha + y)[None]
    vb[pl.ds(idx, 1), pl.ds(y, 1)] = head_value(val, ha + y)[None, None]

    full, full_x = ny // 2 - 1, nx // 2 - 1

    def half(ref, t, way, count):
        if t == 0:
            return ref.at[:, pl.ds(way * (HEAD_DIM // 2), HEAD_DIM // 2)]
        return ref.at[pl.ds(way * (count // 2), count // 2)]

    def a_part(t, slot, way, s):
        part = (ka, va)[t].at[slot]
        return part if s < full else half(part, t, way, ha)

    def b_part(t, slot, way, s):
        part = (kb, vb)[t].at[slot]
        return part if s < full_x else half(part, t, way, ny)

    def a_ring(t, way, s, back):
        sign = 1 - 2 * way
        part = a_part(t, around(y - sign * back, ny), way, s)
        dev = {Y: around(y + sign, ny), X: x, C: c}
        return remote(part, part, ra_send.at[t], ra_recv.at[t, way, s], dev)

    def b_ring(t, way, s, back):
        sign = 1 - 2 * way
        part = b_part(t, around(x - sign * back, nx) * CORES + c, way, s)
        dev = {Y: y, X: around(x + sign, nx), C: c}
        return remote(part, part, rb_send.at[t], rb_recv.at[t, way, s], dev)

    def d_copy(t, way, s, core):
        if s < 0:
            part = (kb, vb)[t].at[x * CORES + core]
        else:
            sign = 1 - 2 * way
            part = b_part(t, around(x - sign * (s + 1), nx) * CORES + core, way, s)
        return remote(part, part, d_send.at[t], d_recv.at[t, 0 if s < 0 else 1 + 2 * s + way], partner)

    def turned(raw):
        return raw.reshape(LANES, HEAD_DIM).astype(F32).T.astype(BF16)

    peers_a, peers_b = pl.ds(0, ha - 1), pl.ds(0, ny - 1)

    def a_pass(t, s):
        for way in ways:
            a_ring(t, way, s, s + 1).wait_recv()
            if s < full:
                a_ring(t, way, s + 1, s + 1).start()

    def b_pass(t, s):
        for way in ways:
            b_ring(t, way, s, s + 1).wait_recv()
            if s < full_x:
                b_ring(t, way, s + 1, s + 1).start()
            d_copy(t, way, s, c).start()

    wait_all(kra.at[peers_a], a_send.at[0])
    a_start(1)
    wait_all(krb.at[peers_b], b_recv.at[0])
    for r in range(b_rows):
        kb[pl.ds(idx, 1), r : r + 1] = turned(krb[r * per : (r + 1) * per])[None, None]
    wait_all(kra.at[peers_a], a_recv.at[0])
    for r in range(a_rows):
        ka[pl.ds(y, 1), r : r + 1] = turned(kra[r * per : (r + 1) * per])[None, None]
    for way in ways:
        a_ring(0, way, 0, 0).start()
    wait_all(segrow.at[peers_a], seg_recv)
    for r in range(a_rows):
        joined = segrow[per * r]
        for g in range(1, per):
            joined = jnp.where(lane >= g * tok, segrow[per * r + g], joined)
        segall[pl.ds(y, 1), r : r + 1, :] = joined[None]
    for _, dev in col:
        remote(segall.at[y], segall.at[y], all_send, all_recv, dev).start()
    wait_all(kra.at[peers_a], a_send.at[1])
    for way in ways:
        b_ring(0, way, 0, 0).start()
    d_copy(0, 0, -1, c).start()
    wait_all(vb.at[0, peers_b], b_recv.at[1])
    for way in ways:
        b_ring(1, way, 0, 0).start()
    d_copy(1, 0, -1, c).start()
    a_start(2)
    wait_all(va.at[0, peers_a], a_recv.at[1])
    for way in ways:
        a_ring(1, way, 0, 0).start()
    a_pass(0, 0)
    wait_all(segall.at[peers_b], all_recv)
    for yy in range(ny):
        for r in range(a_rows):
            hot[yy * requests : (yy + 1) * requests, r * LANES : (r + 1) * LANES] = jnp.where(
                down == segall[yy, r : r + 1, :], 1.0, 0.0
            ).astype(BF16)
    base = -limit
    for yy in range(ny):
        own = hot[yy * requests : (yy + 1) * requests, :]
        own_f = own.astype(F32)
        before = jnp.dot(own, tri[...], preferred_element_type=F32)
        for r in range(a_rows):
            part = slice(r * LANES, (r + 1) * LANES)
            over = jnp.sum(own_f[:, part] * (before[:, part] + base), axis=0, keepdims=True)
            codea[yy, r : r + 1, :] = segall[yy, r : r + 1, :] + jnp.where(over >= 0.0, LATER, 0.0)
        base = base + jnp.sum(own_f, axis=1, keepdims=True)
    for q in range(b_rows):
        for g in range(per):
            line = None
            for h in range(per):
                rows = codea[q * per + h]
                if h != g:
                    rows = pltpu.roll(rows, (h - g) * tok % LANES, 1)
                line = rows if line is None else jnp.where(lane >= h * tok, rows, line)
            codeb[q, g] = line

    def code_a(slot, r):
        return codea[slot, r : r + 1, :]

    def code_b(j, r):
        return codeb[r, lax.rem(j, per), pl.ds(j // per, 1), :]

    def query(raw, code):
        code = turn(code)
        late = code >= LATER
        wide = raw.reshape(LANES, HEAD_DIM).astype(F32)
        inverse = lax.rsqrt(jnp.mean(wide * wide, axis=1, keepdims=True) + EPSILON)
        fresh = wide * inverse * jnp.where(late, query_gain[1:2, :], query_gain[0:1, :])
        seg = jnp.where(late, code - LATER, code)
        same = jnp.where(seg == lane_f, SAME[0], 0.0)
        return jnp.concatenate([fresh.astype(BF16), same.astype(BF16)], axis=1), code

    rate = math.log2(math.e) / math.sqrt(HEAD_DIM)

    def key_work(blocks):
        for n, (raw, code) in enumerate(blocks):
            late = code >= LATER
            wide = raw.astype(F32)
            inverse = lax.rsqrt(jnp.sum(wide * wide, axis=0, keepdims=True) * (1.0 / HEAD_DIM) + EPSILON)
            fresh = wide * inverse * jnp.where(late, gains[1], gains[0])
            part = slice(n * LANES, (n + 1) * LANES)
            kwork[0:HEAD_DIM, part] = fresh.astype(BF16)
            seg = jnp.where(late, code - LATER, code)
            kwork[HEAD_DIM : 2 * HEAD_DIM, part] = jnp.where(deep == seg, SAME[1], 0.0).astype(BF16)
        return len(blocks)

    def soften(q, m, l, acc, count, rows):
        s = jnp.dot(q[rows, :], kwork[:, : count * LANES], preferred_element_type=F32)
        parts = [s[:, n * LANES : (n + 1) * LANES] for n in range(count)]
        top = functools.reduce(jnp.maximum, parts)
        old = m[rows, :]
        new = jnp.maximum(old, jnp.max(top, axis=1, keepdims=True))
        shrink = jnp.exp2((old - new) * rate)
        parts = [jnp.exp2((part - new) * rate) for part in parts]
        m[rows, :] = new
        l[rows, :] = l[rows, :] * shrink + functools.reduce(jnp.add, parts)
        weights = jnp.concatenate([part.astype(BF16) for part in parts], axis=1)
        return weights, acc[rows, :] * shrink

    def attend(q, m, l, acc, blocks, vals):
        count = key_work(blocks)
        step = min(BLOCK, q.shape[0])
        for b in range(q.shape[0] // step):
            rows = slice(b * step, (b + 1) * step)
            weights, kept = soften(q, m, l, acc, count, rows)
            acc[rows, :] = kept + jnp.dot(weights, vals, preferred_element_type=F32)

    def blocks_a(slots):
        return [(ka[slot, r], code_a(slot, r)) for slot in slots for r in range(a_rows)]

    def attend_a(slots):
        vals = jnp.concatenate([va[slot].reshape(row_tok, HEAD_DIM) for slot in slots], axis=0)
        attend(qa, ma, la, acca, blocks_a(slots), vals)

    def attend_b(places):
        ids = [place * CORES + core for place in places for core in range(CORES)]
        blocks = [(kb[j, r], code_b(j, r)) for j in ids for r in range(b_rows)]
        vals = jnp.concatenate([vb[j].reshape(col_tok, HEAD_DIM) for j in ids], axis=0)
        attend(qb, mb, lb, accb, blocks, vals)

    def finish(l, acc):
        return (acc / jnp.sum(l, axis=1, keepdims=True)).astype(BF16)

    def b_slots(s):
        for t in (0, 1):
            for way in ways if s >= 0 else (0,):
                d_copy(t, way, s, 1 - c).wait_recv()
        if s < 0:
            return [x]
        if s < full_x:
            return [around(x - s - 1, nx), around(x + s + 1, nx)]
        return [around(x + nx // 2, nx)]

    b_pass(0, 0)
    b_pass(1, 0)
    wait_all(qrb.at[peers_b], b_recv.at[2])
    wait_all(qra.at[peers_a], a_recv.at[2])
    for r in range(a_rows):
        part = slice(r * LANES, (r + 1) * LANES)
        qa[part, :], cola[part, :] = query(qra[r * per : (r + 1) * per], code_a(y, r))
    for r in range(b_rows):
        part = slice(r * LANES, (r + 1) * LANES)
        qb[part, :], _ = query(qrb[r * per : (r + 1) * per], code_b(idx, r))
    attend_a([y])
    a_pass(1, 0)
    attend_b(b_slots(-1))

    for load in loads[3:]:
        load.wait()
    code = cola[pl.ds(pl.multiple_of(idx * tok, tok), tok), :]
    late = code >= LATER
    seg = jnp.where(late, code - LATER, code)
    total = None
    for kind in range(2):
        pick = jnp.where((seg == lane_f) & (late == (kind == 1)), 1.0, 0.0).astype(BF16)[:, :requests]
        term = jnp.dot(pick, gat[:, kind, :], preferred_element_type=F32)
        total = term if total is None else total + term
    gates[...] = total

    b_step, b_done = 1, -1
    for s in range(full):
        if s + 1 < full:
            a_pass(0, s + 1)
        if b_step <= full_x:
            b_pass(0, b_step)
            b_pass(1, b_step)
            b_step += 1
        attend_a([around(y - s - 1, ny), around(y + s + 1, ny)])
        if s + 1 < full:
            a_pass(1, s + 1)
        if b_done + 1 < b_step:
            b_done += 1
            places = b_slots(b_done)
            attend_b(places)
    for s in range(b_step, full_x + 1):
        b_pass(0, s)
        b_pass(1, s)
    for s in range(b_done + 1, full_x + 1):
        places = b_slots(s)
        attend_b(places)

    ob[...] = finish(lb[...], accb[...]).reshape(ny, tok, HEAD_DIM)
    for j, dev in col:
        remote(ob.at[j], attb.at[y], ob_send, ob_recv, dev).start()
    attb[pl.ds(y, 1)] = ob[pl.ds(y, 1)]

    a_pass(0, full)
    last = around(y + ny // 2, ny)
    count = key_work(blocks_a([last]))
    for b in range(a_rows):
        rows = slice(b * LANES, (b + 1) * LANES)
        held[rows, :], acca[rows, :] = soften(qa, ma, la, acca, count, rows)
    a_pass(1, full)
    oa[...] = finish(
        la[...], acca[...] + jnp.dot(held[...], va[last].reshape(row_tok, HEAD_DIM), preferred_element_type=F32)
    ).reshape(ha, tok, HEAD_DIM)
    for j, dev in row:
        remote(oa.at[j], atta.at[idx], oa_send, oa_recv, dev).start()
    atta[pl.ds(idx, 1)] = oa[pl.ds(idx, 1)]

    wait_all(segrow.at[pl.ds(0, ha - 1)], seg_send)
    wait_all(segall.at[pl.ds(0, ny - 1)], all_send)
    wait_all(kra.at[peers_a], a_send.at[2])
    for n in range(3):
        wait_all(krb.at[peers_b], b_send.at[n])
    for t in (0, 1):
        wait_all((ka, va)[t].at[pl.ds(0, ny - 1)], ra_send.at[t])
        wait_all((kb, vb)[t].at[pl.ds(0, nx - 1)], rb_send.at[t])
        wait_all((kb, vb)[t].at[pl.ds(0, nx)], d_send.at[t])

    wait_all(attb.at[pl.ds(0, ny - 1)], ob_recv)

    def mix(h):
        columns = slice(h * HEAD_DIM, (h + 1) * HEAD_DIM)
        result = atta[h] if h < ha else attb[h - ha]
        out_ref[:, columns] = (
            hid[:, columns].astype(F32) + gates[:, columns] * result.astype(F32)
        ).astype(BF16)

    for h in range(ha, ha + ny):
        mix(h)
    wait_all(attb.at[pl.ds(0, ny - 1)], ob_send)
    wait_all(oa.at[pl.ds(0, ha - 1)], oa_send)
    wait_all(atta.at[pl.ds(0, ha - 1)], oa_recv)
    for h in range(ha):
        mix(h)


def per_device(
    ny, nx, hidden, queries, key_rows, values, query_gain, key_gain, gate_table, segment, text_count
):
    tok, width = hidden.shape
    requests = text_count.shape[0]
    ha = nx * CORES
    row_tok, col_tok = ha * tok, ny * tok
    anywhere = pl.BlockSpec(memory_space=pltpu.HBM)
    vmem = pl.BlockSpec(memory_space=pltpu.VMEM)
    smem = pl.BlockSpec(memory_space=pltpu.SMEM)
    dma = pltpu.SemaphoreType.DMA
    heads = (tok, HEAD_DIM)
    square = (LANES, LANES)
    a_rows, b_rows = row_tok // LANES, col_tok // LANES
    bufs = [
        ((tok, width), BF16),
        ((tok, width), BF16),
        ((tok, width), BF16),
        ((tok, width), BF16),
        ((requests, 2, width), BF16),
        ((ha, *heads), BF16),
        ((ha, *heads), BF16),
        ((ny, *heads), BF16),
        ((ny, *heads), BF16),
        ((ny, a_rows, *square), BF16),
        ((ny, ha, *heads), BF16),
        ((ha, b_rows, *square), BF16),
        ((ha, ny, *heads), BF16),
        ((row_tok, 2 * HEAD_DIM), BF16),
        ((col_tok, 2 * HEAD_DIM), BF16),
        ((ha, 1, LANES), F32),
        ((ny, 8, LANES), F32),
        ((ny, 8, LANES), F32),
        ((b_rows, LANES // tok, 8, LANES), F32),
        ((row_tok, row_tok), BF16),
        ((ny * requests, row_tok), BF16),
        ((row_tok, LANES), F32),
        ((2, *square), F32),
        ((tok, width), F32),
        ((2 * HEAD_DIM, 2 * max(row_tok, 2 * col_tok)), BF16),
        ((row_tok, row_tok), BF16),
        ((row_tok, LANES), F32),
        ((row_tok, LANES), F32),
        ((row_tok, HEAD_DIM), F32),
        ((col_tok, LANES), F32),
        ((col_tok, LANES), F32),
        ((col_tok, HEAD_DIM), F32),
        ((ha, *heads), BF16),
        ((ny, *heads), BF16),
        ((ha, *heads), BF16),
        ((ny, *heads), BF16),
    ]
    steps_y, steps_x = ny // 2, nx // 2
    sems = [(5,), (), (), (), (), (3,), (3,), (3,), (3,)]
    sems += [(2,), (2, 2, steps_y), (2,), (2, 2, steps_x), (2,), (2, 1 + 2 * steps_x), (), (), (), ()]
    return pl.pallas_call(
        functools.partial(kernel, ny, nx, tok, requests),
        out_shape=jax.ShapeDtypeStruct((tok, width), BF16),
        in_specs=[anywhere] * 4 + [vmem] * 2 + [anywhere] + [smem] * 2,
        out_specs=vmem,
        scratch_shapes=[pltpu.VMEM(*buf) for buf in bufs] + [dma(sem) if sem else dma for sem in sems],
        compiler_params=pltpu.CompilerParams(
            collective_id=0, has_side_effects=True, vmem_limit_bytes=VMEM_BYTES
        ),
        name="joint_attention",
    )(hidden, queries, key_rows, values, query_gain, key_gain, gate_table, segment, text_count)


def solution(mesh):
    groups, seq = mesh.shape["groups"], mesh.shape["seq"]
    nx = math.isqrt(seq // CORES)
    ny = seq // CORES // nx
    finer = Mesh(mesh.devices.reshape(groups, ny, nx, CORES), GROUPS_SEQ)
    placed = (
        P(GROUPS_SEQ, None),
        P(GROUPS_SEQ, None),
        P(GROUPS_SEQ, None),
        P(GROUPS_SEQ, None),
        P(),
        P(),
        P("groups", None, None),
        P(GROUPS_SEQ),
        P("groups"),
    )
    return jax.shard_map(
        functools.partial(per_device, ny, nx),
        mesh=finer,
        in_specs=placed,
        out_specs=P(GROUPS_SEQ, None),
        check_vma=False,
    )
```

```python
import functools
import math

import jax
import jax.numpy as jnp
from jax import lax
from jax.experimental import pallas as pl
from jax.experimental.pallas import tpu as pltpu
from jax.sharding import Mesh
from jax.sharding import PartitionSpec as P

HEAD_DIM = 128
LANES = 128
CORES = 2
EPSILON = 1e-06
LOWEST = -1e30
SAME = (128.0, 64.0)
LATER = 64.0
BLOCK = 256
VMEM_BYTES = 40 * 1024 * 1024
Y, X, C = "seq_0", "seq_1", "seq_2"
GROUPS_SEQ = ("groups", Y, X, C)
MESH = pl.DeviceIdType.MESH
F32 = jnp.float32
BF16 = jnp.bfloat16


def kernel(
    ny, nx, tok, requests,
    hidden_hbm, query_hbm, key_hbm, value_hbm, query_gain_hbm, key_gain_hbm, gate_hbm, seg_hbm, text_hbm,
    out_ref,
    hid, que, key, val, gat, kinds, query_gain, key_gain, seg_ref, text_ref,
    kra, qra, krb, qrb, ka, va, kb, vb, qa, qb,
    segrow, segall, codea, codeb, tri, hot, cola, gains, gates, kwork, held,
    ma, la, acca, mb, lb, accb, oa, ob, atta, attb,
    load_sem, seg_send, seg_recv, all_send, all_recv,
    a_send, a_recv, b_send, b_recv, ra_send, ra_recv, rb_send, rb_recv, d_send, d_recv,
    oa_send, oa_recv, ob_send, ob_recv,
):
    ha = nx * CORES
    row_tok, col_tok = ha * tok, ny * tok
    per = LANES // tok
    a_rows, b_rows = row_tok // LANES, col_tok // LANES
    y, x, c = lax.axis_index(Y), lax.axis_index(X), lax.axis_index(C)
    idx = x * CORES + c
    ways = (0, 1)

    loads = [
        pltpu.make_async_copy(src, dst, load_sem.at[n])
        for n, (src, dst) in enumerate(
            [
                (key_hbm, key),
                (value_hbm, val),
                (query_hbm, que),
                (seg_hbm, seg_ref),
                (text_hbm, text_ref),
                (key_gain_hbm, key_gain),
                (query_gain_hbm, query_gain),
                (gate_hbm, gat),
                (hidden_hbm, hid),
            ]
        )
    ]
    for load in loads:
        load.start()

    def around(a, n):
        return lax.rem(a + 2 * n, n)

    row = []
    for dx in sorted(range(nx), key=lambda d: -min(d, nx - d)):
        for dc in range(CORES):
            if dx or dc:
                xx = around(x + dx, nx)
                cc = c if dc == 0 else 1 - c
                row.append((xx * CORES + cc, {Y: y, X: xx, C: cc}))
    col = []
    for dy in sorted(range(1, ny), key=lambda d: -min(d, ny - d)):
        yy = around(y + dy, ny)
        col.append((yy, {Y: yy, X: x, C: c}))
    partner = {Y: y, X: x, C: 1 - c}

    barrier = pltpu.get_barrier_semaphore()
    for _, dev in row + col:
        pl.semaphore_signal(barrier, inc=1, device_id=dev, device_id_type=MESH)

    loads[3].wait()
    lane = lax.broadcasted_iota(jnp.int32, (1, LANES), 1)
    lane_f = lane.astype(F32)
    place = lax.rem(lane, tok)
    mine = jnp.zeros((1, LANES), F32)
    for i in range(tok):
        mine = jnp.where(place == i, seg_ref[i].astype(F32), mine)
    segrow[pl.ds(idx, 1)] = mine.reshape(1, 1, LANES)
    loads[0].wait()
    pl.semaphore_wait(barrier, len(row) + len(col))

    def remote(src, dst, send, recv, dev):
        return pltpu.make_async_remote_copy(
            src_ref=src, dst_ref=dst, send_sem=send, recv_sem=recv, device_id=dev, device_id_type=MESH
        )

    def head(ref, h):
        return ref.at[:, pl.ds(pl.multiple_of(h * HEAD_DIM, HEAD_DIM), HEAD_DIM)]

    def head_value(ref, h):
        return ref[:, pl.ds(pl.multiple_of(h * HEAD_DIM, HEAD_DIM), HEAD_DIM)]

    def wait_all(ref, sem):
        pltpu.make_async_copy(ref, ref, sem).wait()

    tensors = (key, val, que)
    a_in = (kra, va.at[y], qra)
    b_in = (krb, vb.at[idx], qrb)

    def a_start(n):
        for j, dev in row:
            remote(head(tensors[n], j), a_in[n].at[idx], a_send.at[n], a_recv.at[n], dev).start()

    def b_start(n):
        for j, dev in col:
            remote(head(tensors[n], ha + j), b_in[n].at[y], b_send.at[n], b_recv.at[n], dev).start()

    a_start(0)
    b_start(0)
    for _, dev in row:
        remote(segrow.at[idx], segrow.at[idx], seg_send, seg_recv, dev).start()
    for n in (1, 2):
        loads[n].wait()
        b_start(n)

    for load in loads[4:8]:
        load.wait()
    down = lax.broadcasted_iota(jnp.int32, (requests, LANES), 0)
    limit = jnp.zeros((requests, LANES), F32)
    for i in range(requests):
        limit = jnp.where(down == i, text_ref[i].astype(F32), limit)
    down = down.astype(F32)
    deep = lax.broadcasted_iota(jnp.int32, (LANES, LANES), 0).astype(F32)
    for r in range(a_rows):
        first = lax.broadcasted_iota(jnp.int32, (LANES, row_tok), 0) + r * LANES
        second = lax.broadcasted_iota(jnp.int32, (LANES, row_tok), 1)
        tri[r * LANES : (r + 1) * LANES, :] = jnp.where(first < second, 1.0, 0.0).astype(BF16)

    def turn(line):
        return jnp.broadcast_to(line, (LANES, LANES)).T

    for i in range(2):
        gains[i] = turn(key_gain[i : i + 1, :])
    for m, l, acc in ((ma, la, acca), (mb, lb, accb)):
        m[...] = jnp.full(m.shape, LOWEST, F32)
        l[...] = jnp.zeros(l.shape, F32)
        acc[...] = jnp.zeros(acc.shape, F32)

    for kind in range(2):
        kinds[kind] = gat[:, kind, :]

    kra[pl.ds(idx, 1)] = head_value(key, idx)[None]
    qra[pl.ds(idx, 1)] = head_value(que, idx)[None]
    va[pl.ds(y, 1), pl.ds(idx, 1)] = head_value(val, idx)[None, None]
    krb[pl.ds(y, 1)] = head_value(key, ha + y)[None]
    qrb[pl.ds(y, 1)] = head_value(que, ha + y)[None]
    vb[pl.ds(idx, 1), pl.ds(y, 1)] = head_value(val, ha + y)[None, None]

    full, full_x = ny // 2 - 1, nx // 2 - 1

    def half(ref, t, way, count):
        if t == 0:
            return ref.at[:, pl.ds(way * (HEAD_DIM // 2), HEAD_DIM // 2)]
        return ref.at[pl.ds(way * (count // 2), count // 2)]

    def b_part(t, slot, way, s):
        part = (kb, vb)[t].at[slot]
        return part if s < full_x else half(part, t, way, ny)

    def a_ring(t, way, s, back):
        sign = 1 - 2 * way
        slot = around(y - sign * back, ny)
        if t == 0:
            part = ka.at[slot] if s < full else half(ka.at[slot], 0, way, ha)
        else:
            part = half(va.at[slot], 1, t - 1, ha)
        dev = {Y: around(y + sign, ny), X: x, C: c}
        return remote(part, part, ra_send.at[min(t, 1)], ra_recv.at[t, way, s], dev)

    def a_takes(t, way, s):
        return s < full or t == 0 or t - 1 == way

    def a_first(t):
        for way in ways:
            a_ring(t, way, 0, 0).start()

    def b_ring(t, way, s, back):
        sign = 1 - 2 * way
        part = b_part(t, around(x - sign * back, nx) * CORES + c, way, s)
        dev = {Y: y, X: around(x + sign, nx), C: c}
        return remote(part, part, rb_send.at[t], rb_recv.at[t, way, s], dev)

    def d_copy(t, way, s, core):
        if s < 0:
            part = (kb, vb)[t].at[x * CORES + core]
        else:
            sign = 1 - 2 * way
            part = b_part(t, around(x - sign * (s + 1), nx) * CORES + core, way, s)
        return remote(part, part, d_send.at[t], d_recv.at[t, 0 if s < 0 else 1 + 2 * s + way], partner)

    def turned(raw):
        return raw.reshape(LANES, HEAD_DIM).astype(F32).T.astype(BF16)

    peers_a, peers_b = pl.ds(0, ha - 1), pl.ds(0, ny - 1)

    def a_pass(t, s):
        for way in ways:
            if a_takes(t, way, s):
                a_ring(t, way, s, s + 1).wait_recv()
            if s < full and a_takes(t, way, s + 1):
                a_ring(t, way, s + 1, s + 1).start()

    def b_pass(t, s):
        for way in ways:
            b_ring(t, way, s, s + 1).wait_recv()
            if s < full_x:
                b_ring(t, way, s + 1, s + 1).start()
            d_copy(t, way, s, c).start()

    wait_all(kra.at[peers_a], a_send.at[0])
    a_start(1)
    wait_all(kra.at[peers_a], a_recv.at[0])
    for r in range(a_rows):
        ka[pl.ds(y, 1), r : r + 1] = turned(kra[r * per : (r + 1) * per])[None, None]
    a_first(0)
    wait_all(kra.at[peers_a], a_send.at[1])
    a_start(2)
    wait_all(krb.at[peers_b], b_recv.at[0])
    for r in range(b_rows):
        kb[pl.ds(idx, 1), r : r + 1] = turned(krb[r * per : (r + 1) * per])[None, None]
    wait_all(vb.at[0, peers_b], b_recv.at[1])
    for t in (0, 1):
        for way in ways:
            b_ring(t, way, 0, 0).start()
        d_copy(t, 0, -1, c).start()
    wait_all(segrow.at[peers_a], seg_recv)
    for r in range(a_rows):
        joined = segrow[per * r]
        for g in range(1, per):
            joined = jnp.where(lane >= g * tok, segrow[per * r + g], joined)
        segall[pl.ds(y, 1), r : r + 1, :] = joined[None]
    for _, dev in col:
        remote(segall.at[y], segall.at[y], all_send, all_recv, dev).start()
    wait_all(va.at[0, peers_a], a_recv.at[1])
    a_first(1)
    a_pass(0, 0)
    wait_all(segall.at[peers_b], all_recv)
    for yy in range(ny):
        for r in range(a_rows):
            hot[yy * requests : (yy + 1) * requests, r * LANES : (r + 1) * LANES] = jnp.where(
                down == segall[yy, r : r + 1, :], 1.0, 0.0
            ).astype(BF16)
    base = -limit
    for yy in range(ny):
        own = hot[yy * requests : (yy + 1) * requests, :]
        own_f = own.astype(F32)
        before = jnp.dot(own, tri[...], preferred_element_type=F32)
        for r in range(a_rows):
            part = slice(r * LANES, (r + 1) * LANES)
            over = jnp.sum(own_f[:, part] * (before[:, part] + base), axis=0, keepdims=True)
            codea[yy, r : r + 1, :] = segall[yy, r : r + 1, :] + jnp.where(over >= 0.0, LATER, 0.0)
        base = base + jnp.sum(own_f, axis=1, keepdims=True)
    for q in range(b_rows):
        for g in range(per):
            line = None
            for h in range(per):
                rows = codea[q * per + h]
                if h != g:
                    rows = pltpu.roll(rows, (h - g) * tok % LANES, 1)
                line = rows if line is None else jnp.where(lane >= h * tok, rows, line)
            codeb[q, g] = line

    def code_a(slot, r):
        return codea[slot, r : r + 1, :]

    def code_b(j, r):
        return codeb[r, lax.rem(j, per), pl.ds(j // per, 1), :]

    def query(raw, code):
        code = turn(code)
        late = code >= LATER
        wide = raw.reshape(LANES, HEAD_DIM).astype(F32)
        inverse = lax.rsqrt(jnp.mean(wide * wide, axis=1, keepdims=True) + EPSILON)
        fresh = wide * inverse * jnp.where(late, query_gain[1:2, :], query_gain[0:1, :])
        seg = jnp.where(late, code - LATER, code)
        same = jnp.where(seg == lane_f, SAME[0], 0.0)
        return jnp.concatenate([fresh.astype(BF16), same.astype(BF16)], axis=1), code

    rate = math.log2(math.e) / math.sqrt(HEAD_DIM)

    def key_work(blocks):
        for n, (raw, code) in enumerate(blocks):
            late = code >= LATER
            wide = raw.astype(F32)
            inverse = lax.rsqrt(jnp.sum(wide * wide, axis=0, keepdims=True) * (1.0 / HEAD_DIM) + EPSILON)
            fresh = wide * inverse * jnp.where(late, gains[1], gains[0])
            part = slice(n * LANES, (n + 1) * LANES)
            kwork[0:HEAD_DIM, part] = fresh.astype(BF16)
            seg = jnp.where(late, code - LATER, code)
            kwork[HEAD_DIM : 2 * HEAD_DIM, part] = jnp.where(deep == seg, SAME[1], 0.0).astype(BF16)
        return len(blocks)

    def soften(q, m, l, acc, count, rows):
        s = jnp.dot(q[rows, :], kwork[:, : count * LANES], preferred_element_type=F32)
        parts = [s[:, n * LANES : (n + 1) * LANES] for n in range(count)]
        top = functools.reduce(jnp.maximum, parts)
        old = m[rows, :]
        new = jnp.maximum(old, jnp.max(top, axis=1, keepdims=True))
        shrink = jnp.exp2((old - new) * rate)
        parts = [jnp.exp2((part - new) * rate) for part in parts]
        m[rows, :] = new
        l[rows, :] = l[rows, :] * shrink + functools.reduce(jnp.add, parts)
        weights = jnp.concatenate([part.astype(BF16) for part in parts], axis=1)
        return weights, acc[rows, :] * shrink

    def attend(q, m, l, acc, blocks, vals):
        count = key_work(blocks)
        step = min(BLOCK, q.shape[0])
        for b in range(q.shape[0] // step):
            rows = slice(b * step, (b + 1) * step)
            weights, kept = soften(q, m, l, acc, count, rows)
            acc[rows, :] = kept + jnp.dot(weights, vals, preferred_element_type=F32)

    def blocks_a(slots):
        return [(ka[slot, r], code_a(slot, r)) for slot in slots for r in range(a_rows)]

    def keys_a(slots):
        count = key_work(blocks_a(slots))
        step = min(BLOCK, row_tok)
        for b in range(row_tok // step):
            rows = slice(b * step, (b + 1) * step)
            held[rows, : count * LANES], acca[rows, :] = soften(qa, ma, la, acca, count, rows)

    def values_a(slots, rows=slice(None)):
        vals = jnp.concatenate([va[slot].reshape(row_tok, HEAD_DIM) for slot in slots], axis=0)
        return acca[rows, :] + jnp.dot(held[rows, : vals.shape[0]], vals, preferred_element_type=F32)

    def attend_b(places):
        ids = [place * CORES + core for place in places for core in range(CORES)]
        blocks = [(kb[j, r], code_b(j, r)) for j in ids for r in range(b_rows)]
        vals = jnp.concatenate([vb[j].reshape(col_tok, HEAD_DIM) for j in ids], axis=0)
        attend(qb, mb, lb, accb, blocks, vals)

    def finish(l, acc):
        return (acc / jnp.sum(l, axis=1, keepdims=True)).astype(BF16)

    def b_slots(s):
        for t in (0, 1):
            for way in ways if s >= 0 else (0,):
                d_copy(t, way, s, 1 - c).wait_recv()
        if s < 0:
            return [x]
        if s < full_x:
            return [around(x - s - 1, nx), around(x + s + 1, nx)]
        return [around(x + nx // 2, nx)]

    a_first(2)
    wait_all(qrb.at[peers_b], b_recv.at[2])
    wait_all(qra.at[peers_a], a_recv.at[2])
    for r in range(a_rows):
        part = slice(r * LANES, (r + 1) * LANES)
        qa[part, :], cola[part, :] = query(qra[r * per : (r + 1) * per], code_a(y, r))
    for r in range(b_rows):
        part = slice(r * LANES, (r + 1) * LANES)
        qb[part, :], _ = query(qrb[r * per : (r + 1) * per], code_b(idx, r))
    keys_a([y])
    acca[...] = values_a([y])
    b_pass(0, 0)
    b_pass(1, 0)

    b_step, b_done = 1, -2

    def b_next():
        if b_step <= full_x:
            b_pass(0, b_step)
            b_pass(1, b_step)
        return b_step + 1

    def b_attend(upto):
        for b in range(b_done + 1, upto + 1):
            places = b_slots(b)
            attend_b(places)
        return max(b_done, upto)

    for s in range(full):
        slots = [around(y - s - 1, ny), around(y + s + 1, ny)]
        final = s + 1 == full
        if not final:
            a_pass(0, s + 1)
        a_pass(1, s)
        keys_a(slots)
        a_pass(2, s)
        if s > 0:
            b_step = b_next()
        acca[...] = values_a(slots)
        if not final:
            b_done = b_attend(min(s, full_x))
        if s == 0 and not final:
            b_step = b_next()
        if s == 0:
            loads[8].wait()
            code = cola[pl.ds(pl.multiple_of(idx * tok, tok), tok), :]
            late = code >= LATER
            seg = jnp.where(late, code - LATER, code)
            total = 0.0
            for kind in range(2):
                pick = jnp.where((seg == lane_f) & (late == (kind == 1)), 1.0, 0.0).astype(BF16)[:, :requests]
                total = total + jnp.dot(pick, kinds[kind], preferred_element_type=F32)
            gates[...] = total

    while b_step <= full_x:
        b_step = b_next()
    b_done = b_attend(full_x)

    ob[...] = finish(lb[...], accb[...]).reshape(ny, tok, HEAD_DIM)
    for j, dev in col:
        remote(ob.at[j], attb.at[y], ob_send, ob_recv, dev).start()
    attb[pl.ds(y, 1)] = ob[pl.ds(y, 1)]

    a_pass(0, full)
    last = around(y + ny // 2, ny)
    keys_a([last])
    a_pass(1, full)
    a_pass(2, full)
    oa[...] = finish(la[...], values_a([last])).reshape(ha, tok, HEAD_DIM)
    for j, dev in row:
        remote(oa.at[j], atta.at[idx], oa_send, oa_recv, dev).start()
    atta[pl.ds(idx, 1)] = oa[pl.ds(idx, 1)]

    wait_all(segrow.at[pl.ds(0, ha - 1)], seg_send)
    wait_all(segall.at[pl.ds(0, ny - 1)], all_send)
    wait_all(kra.at[peers_a], a_send.at[2])
    for n in range(3):
        wait_all(krb.at[peers_b], b_send.at[n])
    for t in (0, 1):
        wait_all((ka, va)[t].at[pl.ds(0, ny - 1)], ra_send.at[t])
        wait_all((kb, vb)[t].at[pl.ds(0, nx - 1)], rb_send.at[t])
        wait_all((kb, vb)[t].at[pl.ds(0, nx)], d_send.at[t])

    wait_all(attb.at[pl.ds(0, ny - 1)], ob_recv)

    def mix(h):
        columns = slice(h * HEAD_DIM, (h + 1) * HEAD_DIM)
        result = atta[h] if h < ha else attb[h - ha]
        out_ref[:, columns] = (
            hid[:, columns].astype(F32) + gates[:, columns] * result.astype(F32)
        ).astype(BF16)

    for h in range(ha, ha + ny):
        mix(h)
    wait_all(attb.at[pl.ds(0, ny - 1)], ob_send)
    wait_all(oa.at[pl.ds(0, ha - 1)], oa_send)
    wait_all(atta.at[pl.ds(0, ha - 1)], oa_recv)
    for h in range(ha):
        mix(h)


def per_device(
    ny, nx, hidden, queries, key_rows, values, query_gain, key_gain, gate_table, segment, text_count
):
    tok, width = hidden.shape
    requests = text_count.shape[0]
    ha = nx * CORES
    row_tok, col_tok = ha * tok, ny * tok
    anywhere = pl.BlockSpec(memory_space=pltpu.HBM)
    vmem = pl.BlockSpec(memory_space=pltpu.VMEM)
    dma = pltpu.SemaphoreType.DMA
    heads = (tok, HEAD_DIM)
    square = (LANES, LANES)
    a_rows, b_rows = row_tok // LANES, col_tok // LANES
    bufs = [
        ((tok, width), BF16),
        ((tok, width), BF16),
        ((tok, width), BF16),
        ((tok, width), BF16),
        ((requests, 2, width), BF16),
        ((2, requests, width), BF16),
        ((2, HEAD_DIM), F32),
        ((2, HEAD_DIM), F32),
        ((ha, *heads), BF16),
        ((ha, *heads), BF16),
        ((ny, *heads), BF16),
        ((ny, *heads), BF16),
        ((ny, a_rows, *square), BF16),
        ((ny, ha, *heads), BF16),
        ((ha, b_rows, *square), BF16),
        ((ha, ny, *heads), BF16),
        ((row_tok, 2 * HEAD_DIM), BF16),
        ((col_tok, 2 * HEAD_DIM), BF16),
        ((ha, 1, LANES), F32),
        ((ny, 8, LANES), F32),
        ((ny, 8, LANES), F32),
        ((b_rows, LANES // tok, 8, LANES), F32),
        ((row_tok, row_tok), BF16),
        ((ny * requests, row_tok), BF16),
        ((row_tok, LANES), F32),
        ((2, *square), F32),
        ((tok, width), F32),
        ((2 * HEAD_DIM, 2 * max(row_tok, 2 * col_tok)), BF16),
        ((row_tok, 2 * row_tok), BF16),
        ((row_tok, LANES), F32),
        ((row_tok, LANES), F32),
        ((row_tok, HEAD_DIM), F32),
        ((col_tok, LANES), F32),
        ((col_tok, LANES), F32),
        ((col_tok, HEAD_DIM), F32),
        ((ha, *heads), BF16),
        ((ny, *heads), BF16),
        ((ha, *heads), BF16),
        ((ny, *heads), BF16),
    ]
    steps_y, steps_x = ny // 2, nx // 2
    sems = [(9,), (), (), (), (), (3,), (3,), (3,), (3,)]
    sems += [(2,), (3, 2, steps_y), (2,), (2, 2, steps_x), (2,), (2, 1 + 2 * steps_x), (), (), (), ()]
    inputs = [
        pltpu.with_memory_space_constraint(array, pltpu.HBM)
        for array in (
            hidden, queries, key_rows, values, query_gain, key_gain, gate_table, segment, text_count
        )
    ]
    return pl.pallas_call(
        functools.partial(kernel, ny, nx, tok, requests),
        out_shape=jax.ShapeDtypeStruct((tok, width), BF16),
        in_specs=[anywhere] * 9,
        out_specs=vmem,
        scratch_shapes=[pltpu.VMEM(*buf) for buf in bufs[:8]]
        + [pltpu.SMEM((tok,), jnp.int32), pltpu.SMEM((requests,), jnp.int32)]
        + [pltpu.VMEM(*buf) for buf in bufs[8:]]
        + [dma(sem) if sem else dma for sem in sems],
        compiler_params=pltpu.CompilerParams(
            collective_id=0, has_side_effects=True, vmem_limit_bytes=VMEM_BYTES
        ),
        name="joint_attention",
    )(*inputs)


def solution(mesh):
    groups, seq = mesh.shape["groups"], mesh.shape["seq"]
    nx = math.isqrt(seq // CORES)
    ny = seq // CORES // nx
    finer = Mesh(mesh.devices.reshape(groups, ny, nx, CORES), GROUPS_SEQ)
    placed = (
        P(GROUPS_SEQ, None),
        P(GROUPS_SEQ, None),
        P(GROUPS_SEQ, None),
        P(GROUPS_SEQ, None),
        P(),
        P(),
        P("groups", None, None),
        P(GROUPS_SEQ),
        P("groups"),
    )
    return jax.shard_map(
        functools.partial(per_device, ny, nx),
        mesh=finer,
        in_specs=placed,
        out_specs=P(GROUPS_SEQ, None),
        check_vma=False,
    )
```

```python
import functools
import math

import jax
import jax.numpy as jnp
from jax import lax
from jax.experimental import pallas as pl
from jax.experimental.pallas import tpu as pltpu
from jax.sharding import Mesh
from jax.sharding import PartitionSpec as P

HEAD_DIM = 128
LANES = 128
CORES = 2
EPSILON = 1e-06
LOWEST = -1e30
SAME = (128.0, 64.0)
LATER = 64.0
BLOCK = 256
VMEM_BYTES = 40 * 1024 * 1024
Y, X, C = "seq_0", "seq_1", "seq_2"
GROUPS_SEQ = ("groups", Y, X, C)
MESH = pl.DeviceIdType.MESH
F32 = jnp.float32
BF16 = jnp.bfloat16


def kernel(
    ny, nx, tok, requests,
    hidden_hbm, query_hbm, key_hbm, value_hbm, query_gain_hbm, key_gain_hbm, gate_hbm, seg_hbm, text_hbm,
    out_ref,
    hid, que, key, val, gat, kinds, query_gain, key_gain, seg_ref, text_ref,
    kra, qra, krb, qrb, ka, va, kb, vb, qa, qb,
    segrow, segall, codea, codeb, tri, hot, cola, gains, gates, kwork, held,
    ma, la, acca, mb, lb, accb, oa, ob, atta, attb,
    load_sem, seg_send, seg_recv, all_send, all_recv,
    a_send, a_recv, b_send, b_recv, ra_send, ra_recv, rb_send, rb_recv, d_send, d_recv,
    oa_send, oa_recv, ob_send, ob_recv,
):
    ha = nx * CORES
    row_tok, col_tok = ha * tok, ny * tok
    per = LANES // tok
    a_rows, b_rows = row_tok // LANES, col_tok // LANES
    y, x, c = lax.axis_index(Y), lax.axis_index(X), lax.axis_index(C)
    idx = x * CORES + c
    ways = (0, 1)

    loads = [
        pltpu.make_async_copy(src, dst, load_sem.at[n])
        for n, (src, dst) in enumerate(
            [
                (key_hbm, key),
                (value_hbm, val),
                (query_hbm, que),
                (seg_hbm, seg_ref),
                (text_hbm, text_ref),
                (key_gain_hbm, key_gain),
                (query_gain_hbm, query_gain),
                (gate_hbm, gat),
                (hidden_hbm, hid),
            ]
        )
    ]
    for load in loads:
        load.start()

    def around(a, n):
        return lax.rem(a + 2 * n, n)

    row = []
    for dx in sorted(range(nx), key=lambda d: -min(d, nx - d)):
        for dc in range(CORES):
            if dx or dc:
                xx = around(x + dx, nx)
                cc = c if dc == 0 else 1 - c
                row.append((xx * CORES + cc, {Y: y, X: xx, C: cc}))
    col = []
    for dy in sorted(range(1, ny), key=lambda d: -min(d, ny - d)):
        yy = around(y + dy, ny)
        col.append((yy, {Y: yy, X: x, C: c}))
    partner = {Y: y, X: x, C: 1 - c}

    barrier = pltpu.get_barrier_semaphore()
    for _, dev in row + col:
        pl.semaphore_signal(barrier, inc=1, device_id=dev, device_id_type=MESH)

    loads[3].wait()
    lane = lax.broadcasted_iota(jnp.int32, (1, LANES), 1)
    lane_f = lane.astype(F32)
    place = lax.rem(lane, tok)
    mine = jnp.zeros((1, LANES), F32)
    for i in range(tok):
        mine = jnp.where(place == i, seg_ref[i].astype(F32), mine)
    segrow[pl.ds(idx, 1)] = mine.reshape(1, 1, LANES)
    loads[0].wait()
    pl.semaphore_wait(barrier, len(row) + len(col))

    def remote(src, dst, send, recv, dev):
        return pltpu.make_async_remote_copy(
            src_ref=src, dst_ref=dst, send_sem=send, recv_sem=recv, device_id=dev, device_id_type=MESH
        )

    def head(ref, h):
        return ref.at[:, pl.ds(pl.multiple_of(h * HEAD_DIM, HEAD_DIM), HEAD_DIM)]

    def head_value(ref, h):
        return ref[:, pl.ds(pl.multiple_of(h * HEAD_DIM, HEAD_DIM), HEAD_DIM)]

    def wait_all(ref, sem):
        pltpu.make_async_copy(ref, ref, sem).wait()

    tensors = (key, val, que)
    a_in = (kra, va.at[y], qra)
    b_in = (krb, vb.at[idx], qrb)

    def a_start(n):
        for j, dev in row:
            remote(head(tensors[n], j), a_in[n].at[idx], a_send.at[n], a_recv.at[n], dev).start()

    def b_start(n):
        for j, dev in col:
            remote(head(tensors[n], ha + j), b_in[n].at[y], b_send.at[n], b_recv.at[n], dev).start()

    a_start(0)
    b_start(0)
    for _, dev in row:
        remote(segrow.at[idx], segrow.at[idx], seg_send, seg_recv, dev).start()
    for n in (1, 2):
        loads[n].wait()
        b_start(n)

    for load in loads[4:8]:
        load.wait()
    down = lax.broadcasted_iota(jnp.int32, (requests, LANES), 0)
    limit = jnp.zeros((requests, LANES), F32)
    for i in range(requests):
        limit = jnp.where(down == i, text_ref[i].astype(F32), limit)
    down = down.astype(F32)
    deep = lax.broadcasted_iota(jnp.int32, (LANES, LANES), 0).astype(F32)
    for r in range(a_rows):
        first = lax.broadcasted_iota(jnp.int32, (LANES, row_tok), 0) + r * LANES
        second = lax.broadcasted_iota(jnp.int32, (LANES, row_tok), 1)
        tri[r * LANES : (r + 1) * LANES, :] = jnp.where(first < second, 1.0, 0.0).astype(BF16)

    def turn(line):
        return jnp.broadcast_to(line, (LANES, LANES)).T

    for i in range(2):
        gains[i] = turn(key_gain[i : i + 1, :])
    for m, l, acc in ((ma, la, acca), (mb, lb, accb)):
        m[...] = jnp.full(m.shape, LOWEST, F32)
        l[...] = jnp.zeros(l.shape, F32)
        acc[...] = jnp.zeros(acc.shape, F32)

    for kind in range(2):
        kinds[kind] = gat[:, kind, :]

    kra[pl.ds(idx, 1)] = head_value(key, idx)[None]
    qra[pl.ds(idx, 1)] = head_value(que, idx)[None]
    va[pl.ds(y, 1), pl.ds(idx, 1)] = head_value(val, idx)[None, None]
    krb[pl.ds(y, 1)] = head_value(key, ha + y)[None]
    qrb[pl.ds(y, 1)] = head_value(que, ha + y)[None]
    vb[pl.ds(idx, 1), pl.ds(y, 1)] = head_value(val, ha + y)[None, None]

    full, full_x = ny // 2 - 1, nx // 2 - 1

    def half(ref, t, way, count):
        if t == 0:
            return ref.at[:, pl.ds(way * (HEAD_DIM // 2), HEAD_DIM // 2)]
        return ref.at[pl.ds(way * (count // 2), count // 2)]

    def b_part(t, slot, way, s):
        part = (kb, vb)[t].at[slot]
        return part if s < full_x else half(part, t, way, ny)

    def a_ring(t, way, s, back):
        sign = 1 - 2 * way
        slot = around(y - sign * back, ny)
        part = half((ka, va)[t // 2].at[slot], t // 2, t % 2, ha)
        dev = {Y: around(y + sign, ny), X: x, C: c}
        return remote(part, part, ra_send.at[t], ra_recv.at[t, way, s], dev)

    def a_takes(t, way, s):
        return s < full or t % 2 == way

    def a_first(t):
        for way in ways:
            a_ring(t, way, 0, 0).start()

    def a_left(t, halves):
        size = ha // 2 * tok * HEAD_DIM // held.shape[1]
        wait_all(held.at[pl.ds(0, halves * size)], ra_send.at[t])

    def b_ring(t, way, s, back):
        sign = 1 - 2 * way
        part = b_part(t, around(x - sign * back, nx) * CORES + c, way, s)
        dev = {Y: y, X: around(x + sign, nx), C: c}
        return remote(part, part, rb_send.at[t], rb_recv.at[t, way, s], dev)

    def d_copy(t, way, s, core):
        if s < 0:
            part = (kb, vb)[t].at[x * CORES + core]
        else:
            sign = 1 - 2 * way
            part = b_part(t, around(x - sign * (s + 1), nx) * CORES + core, way, s)
        return remote(part, part, d_send.at[t], d_recv.at[t, 0 if s < 0 else 1 + 2 * s + way], partner)

    def turned(raw):
        return raw.reshape(LANES, HEAD_DIM).astype(F32).T.astype(BF16)

    peers_a, peers_b = pl.ds(0, ha - 1), pl.ds(0, ny - 1)

    def a_pass(t, s):
        for way in ways:
            if a_takes(t, way, s):
                a_ring(t, way, s, s + 1).wait_recv()
            if s < full and a_takes(t, way, s + 1):
                a_ring(t, way, s + 1, s + 1).start()

    def b_pass(t, s):
        for way in ways:
            b_ring(t, way, s, s + 1).wait_recv()
            if s < full_x:
                b_ring(t, way, s + 1, s + 1).start()
            d_copy(t, way, s, c).start()

    wait_all(kra.at[peers_a], a_send.at[0])
    a_start(1)
    wait_all(kra.at[peers_a], a_recv.at[0])
    for r in range(a_rows):
        ka[pl.ds(y, 1), r : r + 1] = turned(kra[r * per : (r + 1) * per])[None, None]
    a_first(0)
    wait_all(kra.at[peers_a], a_send.at[1])
    a_start(2)
    wait_all(krb.at[peers_b], b_recv.at[0])
    for r in range(b_rows):
        kb[pl.ds(idx, 1), r : r + 1] = turned(krb[r * per : (r + 1) * per])[None, None]
    wait_all(vb.at[0, peers_b], b_recv.at[1])
    for t in (0, 1):
        for way in ways:
            b_ring(t, way, 0, 0).start()
        d_copy(t, 0, -1, c).start()
    a_first(1)
    wait_all(segrow.at[peers_a], seg_recv)
    for r in range(a_rows):
        joined = segrow[per * r]
        for g in range(1, per):
            joined = jnp.where(lane >= g * tok, segrow[per * r + g], joined)
        segall[pl.ds(y, 1), r : r + 1, :] = joined[None]
    for _, dev in col:
        remote(segall.at[y], segall.at[y], all_send, all_recv, dev).start()
    wait_all(va.at[0, peers_a], a_recv.at[1])
    a_first(2)
    a_pass(0, 0)
    a_pass(1, 0)
    a_first(3)
    wait_all(segall.at[peers_b], all_recv)
    for yy in range(ny):
        for r in range(a_rows):
            hot[yy * requests : (yy + 1) * requests, r * LANES : (r + 1) * LANES] = jnp.where(
                down == segall[yy, r : r + 1, :], 1.0, 0.0
            ).astype(BF16)
    base = -limit
    for yy in range(ny):
        own = hot[yy * requests : (yy + 1) * requests, :]
        own_f = own.astype(F32)
        before = jnp.dot(own, tri[...], preferred_element_type=F32)
        for r in range(a_rows):
            part = slice(r * LANES, (r + 1) * LANES)
            over = jnp.sum(own_f[:, part] * (before[:, part] + base), axis=0, keepdims=True)
            codea[yy, r : r + 1, :] = segall[yy, r : r + 1, :] + jnp.where(over >= 0.0, LATER, 0.0)
        base = base + jnp.sum(own_f, axis=1, keepdims=True)
    for q in range(b_rows):
        for g in range(per):
            line = None
            for h in range(per):
                rows = codea[q * per + h]
                if h != g:
                    rows = pltpu.roll(rows, (h - g) * tok % LANES, 1)
                line = rows if line is None else jnp.where(lane >= h * tok, rows, line)
            codeb[q, g] = line

    def code_a(slot, r):
        return codea[slot, r : r + 1, :]

    def code_b(j, r):
        return codeb[r, lax.rem(j, per), pl.ds(j // per, 1), :]

    def query(raw, code):
        code = turn(code)
        late = code >= LATER
        wide = raw.reshape(LANES, HEAD_DIM).astype(F32)
        inverse = lax.rsqrt(jnp.mean(wide * wide, axis=1, keepdims=True) + EPSILON)
        fresh = wide * inverse * jnp.where(late, query_gain[1:2, :], query_gain[0:1, :])
        seg = jnp.where(late, code - LATER, code)
        same = jnp.where(seg == lane_f, SAME[0], 0.0)
        return jnp.concatenate([fresh.astype(BF16), same.astype(BF16)], axis=1), code

    rate = math.log2(math.e) / math.sqrt(HEAD_DIM)

    def key_work(blocks):
        for n, (raw, code) in enumerate(blocks):
            late = code >= LATER
            wide = raw.astype(F32)
            inverse = lax.rsqrt(jnp.sum(wide * wide, axis=0, keepdims=True) * (1.0 / HEAD_DIM) + EPSILON)
            fresh = wide * inverse * jnp.where(late, gains[1], gains[0])
            part = slice(n * LANES, (n + 1) * LANES)
            kwork[0:HEAD_DIM, part] = fresh.astype(BF16)
            seg = jnp.where(late, code - LATER, code)
            kwork[HEAD_DIM : 2 * HEAD_DIM, part] = jnp.where(deep == seg, SAME[1], 0.0).astype(BF16)
        return len(blocks)

    def soften(q, m, l, acc, count, rows):
        s = jnp.dot(q[rows, :], kwork[:, : count * LANES], preferred_element_type=F32)
        parts = [s[:, n * LANES : (n + 1) * LANES] for n in range(count)]
        top = functools.reduce(jnp.maximum, parts)
        old = m[rows, :]
        new = jnp.maximum(old, jnp.max(top, axis=1, keepdims=True))
        shrink = jnp.exp2((old - new) * rate)
        parts = [jnp.exp2((part - new) * rate) for part in parts]
        m[rows, :] = new
        l[rows, :] = l[rows, :] * shrink + functools.reduce(jnp.add, parts)
        weights = jnp.concatenate([part.astype(BF16) for part in parts], axis=1)
        return weights, acc[rows, :] * shrink

    def attend(q, m, l, acc, blocks, vals):
        count = key_work(blocks)
        step = min(BLOCK, q.shape[0])
        for b in range(q.shape[0] // step):
            rows = slice(b * step, (b + 1) * step)
            weights, kept = soften(q, m, l, acc, count, rows)
            acc[rows, :] = kept + jnp.dot(weights, vals, preferred_element_type=F32)

    def blocks_a(slots):
        return [(ka[slot, r], code_a(slot, r)) for slot in slots for r in range(a_rows)]

    def keys_a(slots):
        count = key_work(blocks_a(slots))
        step = min(BLOCK, row_tok)
        for b in range(row_tok // step):
            rows = slice(b * step, (b + 1) * step)
            held[rows, : count * LANES], acca[rows, :] = soften(qa, ma, la, acca, count, rows)

    def values_a(slots, rows=slice(None)):
        vals = jnp.concatenate([va[slot].reshape(row_tok, HEAD_DIM) for slot in slots], axis=0)
        return acca[rows, :] + jnp.dot(held[rows, : vals.shape[0]], vals, preferred_element_type=F32)

    def attend_b(places):
        ids = [place * CORES + core for place in places for core in range(CORES)]
        blocks = [(kb[j, r], code_b(j, r)) for j in ids for r in range(b_rows)]
        vals = jnp.concatenate([vb[j].reshape(col_tok, HEAD_DIM) for j in ids], axis=0)
        attend(qb, mb, lb, accb, blocks, vals)

    def finish(l, acc):
        return (acc / jnp.sum(l, axis=1, keepdims=True)).astype(BF16)

    def b_slots(s):
        for t in (0, 1):
            for way in ways if s >= 0 else (0,):
                d_copy(t, way, s, 1 - c).wait_recv()
        if s < 0:
            return [x]
        if s < full_x:
            return [around(x - s - 1, nx), around(x + s + 1, nx)]
        return [around(x + nx // 2, nx)]

    wait_all(qrb.at[peers_b], b_recv.at[2])
    wait_all(qra.at[peers_a], a_recv.at[2])
    for r in range(a_rows):
        part = slice(r * LANES, (r + 1) * LANES)
        qa[part, :], cola[part, :] = query(qra[r * per : (r + 1) * per], code_a(y, r))
    for r in range(b_rows):
        part = slice(r * LANES, (r + 1) * LANES)
        qb[part, :], _ = query(qrb[r * per : (r + 1) * per], code_b(idx, r))
    keys_a([y])
    acca[...] = values_a([y])
    b_pass(0, 0)
    b_pass(1, 0)

    b_step, b_done = 1, -2

    def b_next():
        if b_step <= full_x:
            b_pass(0, b_step)
            b_pass(1, b_step)
        return b_step + 1

    def b_attend(upto):
        for b in range(b_done + 1, upto + 1):
            places = b_slots(b)
            attend_b(places)
        return max(b_done, upto)

    for s in range(full):
        slots = [around(y - s - 1, ny), around(y + s + 1, ny)]
        final = s + 1 == full
        if not final:
            a_pass(0, s + 1)
            a_pass(1, s + 1)
        a_pass(2, s)
        keys_a(slots)
        a_pass(3, s)
        if s > 0 and not final:
            b_step = b_next()
        acca[...] = values_a(slots)
        if final:
            while b_step <= full_x:
                b_step = b_next()
        b_done = b_attend(full_x if final else min(s, b_step - 1, full_x))
        if s == 0 and not final:
            b_step = b_next()
        if s == 0:
            loads[8].wait()
            code = cola[pl.ds(pl.multiple_of(idx * tok, tok), tok), :]
            late = code >= LATER
            seg = jnp.where(late, code - LATER, code)
            total = 0.0
            for kind in range(2):
                pick = jnp.where((seg == lane_f) & (late == (kind == 1)), 1.0, 0.0).astype(BF16)[:, :requests]
                total = total + jnp.dot(pick, kinds[kind], preferred_element_type=F32)
            gates[...] = total

    ob[...] = finish(lb[...], accb[...]).reshape(ny, tok, HEAD_DIM)
    for j, dev in col:
        remote(ob.at[j], attb.at[y], ob_send, ob_recv, dev).start()
    attb[pl.ds(y, 1)] = ob[pl.ds(y, 1)]

    a_pass(0, full)
    a_pass(1, full)
    last = around(y + ny // 2, ny)
    keys_a([last])
    a_pass(2, full)
    a_pass(3, full)
    oa[...] = finish(la[...], values_a([last])).reshape(ha, tok, HEAD_DIM)
    for j, dev in row:
        remote(oa.at[j], atta.at[idx], oa_send, oa_recv, dev).start()
    atta[pl.ds(idx, 1)] = oa[pl.ds(idx, 1)]

    wait_all(segrow.at[pl.ds(0, ha - 1)], seg_send)
    wait_all(segall.at[pl.ds(0, ny - 1)], all_send)
    wait_all(kra.at[peers_a], a_send.at[2])
    for n in range(3):
        wait_all(krb.at[peers_b], b_send.at[n])
    for t in range(4):
        a_left(t, 2 * full + 1)
    for t in (0, 1):
        wait_all((kb, vb)[t].at[pl.ds(0, nx - 1)], rb_send.at[t])
        wait_all((kb, vb)[t].at[pl.ds(0, nx)], d_send.at[t])

    wait_all(attb.at[pl.ds(0, ny - 1)], ob_recv)

    def mix(h):
        columns = slice(h * HEAD_DIM, (h + 1) * HEAD_DIM)
        result = atta[h] if h < ha else attb[h - ha]
        out_ref[:, columns] = (
            hid[:, columns].astype(F32) + gates[:, columns] * result.astype(F32)
        ).astype(BF16)

    for h in range(ha, ha + ny):
        mix(h)
    wait_all(attb.at[pl.ds(0, ny - 1)], ob_send)
    wait_all(oa.at[pl.ds(0, ha - 1)], oa_send)
    wait_all(atta.at[pl.ds(0, ha - 1)], oa_recv)
    for h in range(ha):
        mix(h)


def per_device(
    ny, nx, hidden, queries, key_rows, values, query_gain, key_gain, gate_table, segment, text_count
):
    tok, width = hidden.shape
    requests = text_count.shape[0]
    ha = nx * CORES
    row_tok, col_tok = ha * tok, ny * tok
    anywhere = pl.BlockSpec(memory_space=pltpu.HBM)
    vmem = pl.BlockSpec(memory_space=pltpu.VMEM)
    dma = pltpu.SemaphoreType.DMA
    heads = (tok, HEAD_DIM)
    square = (LANES, LANES)
    a_rows, b_rows = row_tok // LANES, col_tok // LANES
    bufs = [
        ((tok, width), BF16),
        ((tok, width), BF16),
        ((tok, width), BF16),
        ((tok, width), BF16),
        ((requests, 2, width), BF16),
        ((2, requests, width), BF16),
        ((2, HEAD_DIM), F32),
        ((2, HEAD_DIM), F32),
        ((ha, *heads), BF16),
        ((ha, *heads), BF16),
        ((ny, *heads), BF16),
        ((ny, *heads), BF16),
        ((ny, a_rows, *square), BF16),
        ((ny, ha, *heads), BF16),
        ((ha, b_rows, *square), BF16),
        ((ha, ny, *heads), BF16),
        ((row_tok, 2 * HEAD_DIM), BF16),
        ((col_tok, 2 * HEAD_DIM), BF16),
        ((ha, 1, LANES), F32),
        ((ny, 8, LANES), F32),
        ((ny, 8, LANES), F32),
        ((b_rows, LANES // tok, 8, LANES), F32),
        ((row_tok, row_tok), BF16),
        ((ny * requests, row_tok), BF16),
        ((row_tok, LANES), F32),
        ((2, *square), F32),
        ((tok, width), F32),
        ((2 * HEAD_DIM, 2 * max(row_tok, 2 * col_tok)), BF16),
        ((row_tok, 2 * row_tok), BF16),
        ((row_tok, LANES), F32),
        ((row_tok, LANES), F32),
        ((row_tok, HEAD_DIM), F32),
        ((col_tok, LANES), F32),
        ((col_tok, LANES), F32),
        ((col_tok, HEAD_DIM), F32),
        ((ha, *heads), BF16),
        ((ny, *heads), BF16),
        ((ha, *heads), BF16),
        ((ny, *heads), BF16),
    ]
    steps_y, steps_x = ny // 2, nx // 2
    sems = [(9,), (), (), (), (), (3,), (3,), (3,), (3,)]
    sems += [(4,), (4, 2, steps_y), (2,), (2, 2, steps_x), (2,), (2, 1 + 2 * steps_x), (), (), (), ()]
    inputs = [
        pltpu.with_memory_space_constraint(array, pltpu.HBM)
        for array in (
            hidden, queries, key_rows, values, query_gain, key_gain, gate_table, segment, text_count
        )
    ]
    return pl.pallas_call(
        functools.partial(kernel, ny, nx, tok, requests),
        out_shape=jax.ShapeDtypeStruct((tok, width), BF16),
        in_specs=[anywhere] * 9,
        out_specs=vmem,
        scratch_shapes=[pltpu.VMEM(*buf) for buf in bufs[:8]]
        + [pltpu.SMEM((tok,), jnp.int32), pltpu.SMEM((requests,), jnp.int32)]
        + [pltpu.VMEM(*buf) for buf in bufs[8:]]
        + [dma(sem) if sem else dma for sem in sems],
        compiler_params=pltpu.CompilerParams(
            collective_id=0, has_side_effects=True, vmem_limit_bytes=VMEM_BYTES
        ),
        name="joint_attention",
    )(*inputs)


def solution(mesh):
    groups, seq = mesh.shape["groups"], mesh.shape["seq"]
    nx = math.isqrt(seq // CORES)
    ny = seq // CORES // nx
    finer = Mesh(mesh.devices.reshape(groups, ny, nx, CORES), GROUPS_SEQ)
    placed = (
        P(GROUPS_SEQ, None),
        P(GROUPS_SEQ, None),
        P(GROUPS_SEQ, None),
        P(GROUPS_SEQ, None),
        P(),
        P(),
        P("groups", None, None),
        P(GROUPS_SEQ),
        P("groups"),
    )
    return jax.shard_map(
        functools.partial(per_device, ny, nx),
        mesh=finer,
        in_specs=placed,
        out_specs=P(GROUPS_SEQ, None),
        check_vma=False,
    )
```
